32 devices in a mesh: gx: 2 (over x), gy: 4 (over y, core), gz: 4 (over z).
Axes of the slice: x: 2, y: 2, z: 4, core: 2. Of those that a mesh axis runs over, the one named last changes fastest.
Arguments:
- conserved: float32 [5, 16, 32, 256], P(None, 'gz', 'gy', 'gx'), may hold values from -3 to 12, as said below
- metrics: float32 [9, 16, 32, 256], P(None, 'gz', 'gy', 'gx'), may hold values from -0.6 to 2, as said below
- inv_volume: float32 [16, 32, 256], P('gz', 'gy', 'gx'), may hold values from 0.5 to 2
- wake_donor: int32 [256], P('gx'), may hold values from -1 to 255, as said below
Outputs:
- section_state: float32 [5, 16, 32, 256], P(None, 'gz', 'gy', 'gx')
- time_rate: float32 [5, 16, 32, 256], P(None, 'gz', 'gy', 'gx')
The draws below stay inside these ranges and needn't reach their ends.
Inputs may be any that keep to these rules, and one draw needn't show every extreme that they name: `conserved`: each cell holds density rho of 0.5 to 2, pressure p of 0.5 to 2 and velocity components u of -1.5 to 1.5 as (rho, rho u, p / 0.4 + rho |u|^2 / 2). `metrics`: in each cell, row d (entries 3 d to 3 d + 2) has its entry 3 d + d between 0.5 and 2 and its other two entries at most 0.3 times that entry in magnitude. wake_donor[i] is either 256 - 1 - i or -1, and wake_donor[i] >= 0 exactly where wake_donor[255 - i] >= 0.
All inputs are finite; a program needn't handle non-finite values.
Results may differ from the reference program's by a relative error of at most 0.0001.
Values sent between devices are 32-bit elements; how exact they have to be, the bound alone decides.
A program may use at most 64 MiB of HBM per device.

```python
import math
import jax
import jax.numpy as jnp
from jax import lax

CY = 8
CZ = 4
NX = 256
NY = 32
NZ = 16


def draw_conserved(key, part):
    subkeys = jax.random.split(key, 3)
    grid_shape = (NZ, NY, NX)
    density = jnp.exp(jax.random.uniform(subkeys[0], grid_shape, jnp.float32, -0.6931, 0.6931))
    pressure = jnp.exp(jax.random.uniform(subkeys[1], grid_shape, jnp.float32, -0.6931, 0.6931))
    velocity = jnp.clip(0.5 * jax.random.normal(subkeys[2], (3,) + grid_shape, jnp.float32), -1.5, 1.5)
    energy = pressure / 0.4 + 0.5 * density * jnp.sum(velocity * velocity, axis=0)
    return jnp.concatenate([density[None], density[None] * velocity, energy[None]], axis=0).astype(jnp.float32)


def draw_metrics(key, part):
    subkeys = jax.random.split(key, 2)
    grid_shape = (NZ, NY, NX)
    diagonal = jnp.exp(jax.random.uniform(subkeys[0], (3,) + grid_shape, jnp.float32, -0.6931, 0.6931))
    ratios = jax.random.uniform(subkeys[1], (3, 3) + grid_shape, jnp.float32, -0.3, 0.3)
    entries = []
    for direction in range(3):
        for component in range(3):
            if component == direction:
                entries.append(diagonal[direction])
            else:
                entries.append(ratios[direction, component] * diagonal[direction])
    return jnp.stack(entries).astype(jnp.float32)


def draw_wake_donor(key, part):
    own_key = jax.random.fold_in(key, 4177)
    half_flags = jax.random.randint(own_key, (NX // 2,), 0, 2).astype(jnp.int32)
    flags = jnp.concatenate([half_flags, half_flags[::-1]], axis=0)
    column = jnp.arange(NX, dtype=jnp.int32)
    return jnp.where(flags > 0, NX - 1 - column, -1).astype(jnp.int32)


def steps_of(rng, shape, shards, low, top_value):
    def one(dim, parts):
        steps = jax.random.uniform(jax.random.fold_in(jax.random.fold_in(rng, 6), dim), (parts,), jnp.float32, low / len(shards), top_value / len(shards))
        return jnp.repeat(jnp.exp(steps), shape[dim] // parts).reshape((-1,) + (1,) * (len(shape) - dim - 1))

    gain = one(*shards[0])
    for cut in shards[1:]:
        gain = gain * one(*cut)
    return gain


def setup_inputs(seed: int = 0) -> dict:
    streams_of = jax.random.split(jax.random.key(seed), 5)
    return {
        "conserved": draw_conserved(jax.random.fold_in(streams_of[4], 71), 0),
        "metrics": draw_metrics(jax.random.fold_in(streams_of[4], 71), 0),
        "inv_volume": jnp.clip(jnp.exp(math.log(2.0) - 1.3862944 * jax.random.uniform(streams_of[2], (NZ, NY, NX), jnp.float32) ** steps_of(streams_of[2], (NZ, NY, NX), ((0, 4), (1, 4), (2, 2)), -0.2, 0.2)), 0.5, 2.0),
        "wake_donor": draw_wake_donor(jax.random.fold_in(streams_of[4], 71), 0),
    }


GAMMA = 1.4
WENO_EPS = 1e-06
STEP_SIZE = 0.08

def slab_of(values, start, amount, axis):
    return lax.slice_in_dim(values, start, start + amount, axis=values.ndim + axis)

def cross_of(first, second):
    return [first[1] * second[2] - first[2] * second[1], first[2] * second[0] - first[0] * second[2], first[0] * second[1] - first[1] * second[0]]

def inner_of(first, second):
    return first[0] * second[0] + first[1] * second[1] + first[2] * second[2]

def cell_terms(fields, metric_row):
    density = fields[0]
    velocity = fields[1:4] / density
    kinetic = 0.5 * lax.optimization_barrier(jnp.sum(fields[1:4] * velocity, axis=0))
    pressure = (GAMMA - 1.0) * (fields[4] - kinetic)
    contra = lax.optimization_barrier(jnp.sum(metric_row * velocity, axis=0))
    fluxes = jnp.stack([fields[0] * contra, fields[1] * contra + metric_row[0] * pressure, fields[2] * contra + metric_row[1] * pressure, fields[3] * contra + metric_row[2] * pressure, (fields[4] + pressure) * contra])
    sound_speed = jnp.sqrt(GAMMA * pressure / density)
    speeds = jnp.abs(contra) + sound_speed * jnp.sqrt(lax.optimization_barrier(jnp.sum(metric_row * metric_row, axis=0)))
    primitive = jnp.concatenate([density[None], velocity, pressure[None]], axis=0)
    return (primitive, fluxes, speeds)

def eigen_pair(state, metric_row, pick):
    density = state[0]
    velocity = [state[1], state[2], state[3]]
    pressure = state[4]
    row_size = jnp.sqrt(metric_row[0] ** 2 + metric_row[1] ** 2 + metric_row[2] ** 2)
    normal = [metric_row[member] / row_size for member in range(3)]
    axis_unit = [1.0 if member == pick else 0.0 for member in range(3)]
    raw_cross = cross_of(normal, axis_unit)
    raw_size = jnp.sqrt(raw_cross[0] ** 2 + raw_cross[1] ** 2 + raw_cross[2] ** 2)
    tangent = [raw_cross[member] / raw_size for member in range(3)]
    binormal = cross_of(normal, tangent)
    sound_speed = jnp.sqrt(GAMMA * pressure / density)
    inverse = 1.0 / sound_speed
    kinetic = 0.5 * inner_of(velocity, velocity)
    enthalpy = GAMMA / (GAMMA - 1.0) * pressure / density + kinetic
    normal_speed = inner_of(normal, velocity)
    tangent_speed = inner_of(tangent, velocity)
    binormal_speed = inner_of(binormal, velocity)
    factor = (GAMMA - 1.0) * inverse * inverse
    scaled = factor * kinetic
    left_rows = [[0.5 * (scaled + normal_speed * inverse)] + [0.5 * (-factor * velocity[member] - normal[member] * inverse) for member in range(3)] + [0.5 * factor], [1.0 - scaled] + [factor * velocity[member] for member in range(3)] + [-factor], [-tangent_speed] + tangent + [0.0], [-binormal_speed] + binormal + [0.0], [0.5 * (scaled - normal_speed * inverse)] + [0.5 * (-factor * velocity[member] + normal[member] * inverse) for member in range(3)] + [0.5 * factor]]
    right_columns = [[1.0] + [velocity[member] - sound_speed * normal[member] for member in range(3)] + [enthalpy - sound_speed * normal_speed], [1.0] + velocity + [kinetic], [0.0] + tangent + [tangent_speed], [0.0] + binormal + [binormal_speed], [1.0] + [velocity[member] + sound_speed * normal[member] for member in range(3)] + [enthalpy + sound_speed * normal_speed]]
    return (left_rows, right_columns)

def project_left(matrix, vector):
    return jnp.stack([sum((matrix[member][second] * vector[second] for second in range(5))) for member in range(5)])

def apply_right(matrix, vector):
    return jnp.stack([sum((matrix[second][member] * vector[second] for second in range(5))) for member in range(5)])

def weno_side(stencil):
    far_left, near_left, center, near_right, far_right = stencil
    guess_zero = (2.0 * far_left - 7.0 * near_left + 11.0 * center) / 6.0
    guess_one = (-near_left + 5.0 * center + 2.0 * near_right) / 6.0
    guess_two = (2.0 * center + 5.0 * near_right - far_right) / 6.0
    smooth_zero = 13.0 / 12.0 * (far_left - 2.0 * near_left + center) ** 2 + 0.25 * (far_left - 4.0 * near_left + 3.0 * center) ** 2
    smooth_one = 13.0 / 12.0 * (near_left - 2.0 * center + near_right) ** 2 + 0.25 * (near_left - near_right) ** 2
    smooth_two = 13.0 / 12.0 * (center - 2.0 * near_right + far_right) ** 2 + 0.25 * (3.0 * center - 4.0 * near_right + far_right) ** 2
    weight_zero = 0.1 / (WENO_EPS + smooth_zero) ** 2
    weight_one = 0.6 / (WENO_EPS + smooth_one) ** 2
    weight_two = 0.3 / (WENO_EPS + smooth_two) ** 2
    return (weight_zero * guess_zero + weight_one * guess_one + weight_two * guess_two) / (weight_zero + weight_one + weight_two)

def interface_flux(fields, metric_row, axis, pick):
    primitive, fluxes, speeds = cell_terms(fields, metric_row)
    faces_count = fields.shape[fields.ndim + axis] - 5
    mean_state = 0.5 * (slab_of(primitive, 2, faces_count, axis) + slab_of(primitive, 3, faces_count, axis))
    mean_row = 0.5 * (slab_of(metric_row, 2, faces_count, axis) + slab_of(metric_row, 3, faces_count, axis))
    left_rows, right_columns = eigen_pair(mean_state, mean_row, pick)
    max_speed = slab_of(speeds, 0, faces_count, axis)
    for offset in range(1, 6):
        max_speed = jnp.maximum(max_speed, slab_of(speeds, offset, faces_count, axis))
    upwind = []
    downwind = []
    for offset in range(6):
        state_chars = project_left(left_rows, slab_of(fields, offset, faces_count, axis))
        flux_chars = project_left(left_rows, slab_of(fluxes, offset, faces_count, axis))
        upwind.append(0.5 * (flux_chars + max_speed * state_chars))
        downwind.append(0.5 * (flux_chars - max_speed * state_chars))
    combined = weno_side(upwind[0:5]) + weno_side(downwind[5:0:-1])
    return apply_right(right_columns, combined)

def divergence(fields, metric_row, axis, pick):
    face_flux = interface_flux(fields, metric_row, axis, pick)
    cells_count = face_flux.shape[face_flux.ndim + axis] - 1
    return slab_of(face_flux, 1, cells_count, axis) - slab_of(face_flux, 0, cells_count, axis)

def blocked(fields, metric_row, axis, pick, block_dim, block):
    pieces = fields.shape[block_dim] // block

    def one_block(start):
        flow_part = lax.dynamic_slice_in_dim(fields, start, block, block_dim)
        row_part = lax.dynamic_slice_in_dim(metric_row, start, block, block_dim)
        return divergence(flow_part, row_part, axis, pick)
    starts = jnp.arange(pieces, dtype=jnp.int32) * block
    stacked = lax.map(one_block, starts)
    moved = jnp.moveaxis(stacked, 0, block_dim)
    dims = list(moved.shape)
    merged = dims[:block_dim] + [pieces * block] + dims[block_dim + 2:]
    return moved.reshape(merged)

def reference(conserved, metrics, inv_volume, wake_donor):
    edge_pad = ((0, 0), (0, 0), (0, 0), (3, 3))
    stream_flow = jnp.pad(conserved, edge_pad, mode='edge')
    stream_row = jnp.pad(metrics[0:3], edge_pad, mode='edge')
    momentum_sign = jnp.array([1.0, -1.0, -1.0, -1.0, 1.0], dtype=jnp.float32)[:, None, None, None]
    below_wall = conserved[:, :, 2::-1, :]
    below_row = metrics[3:6, :, 2::-1, :]
    is_wake = wake_donor >= 0
    source_column = jnp.where(is_wake, wake_donor, 0).astype(jnp.int32)
    low_flow = jnp.where(is_wake, jnp.take(below_wall, source_column, axis=3), below_wall * momentum_sign)
    low_row = jnp.where(is_wake, jnp.take(below_row, source_column, axis=3), below_row)
    normal_flow = jnp.concatenate([low_flow, conserved, jnp.repeat(conserved[:, :, -1:, :], 3, axis=2)], axis=2)
    normal_row = jnp.concatenate([low_row, metrics[3:6], jnp.repeat(metrics[3:6, :, -1:, :], 3, axis=2)], axis=2)
    span_flow = jnp.concatenate([conserved[:, -3:], conserved, conserved[:, :3]], axis=1)
    span_metric = metrics[6:9]
    span_row = jnp.concatenate([span_metric[:, -3:], span_metric, span_metric[:, :3]], axis=1)
    summed = blocked(stream_flow, stream_row, -1, 1, 1, CZ)
    summed = summed + blocked(normal_flow, normal_row, -2, 2, 1, CZ)
    summed = summed + blocked(span_flow, span_row, -3, 0, 2, CY)
    time_rate = -inv_volume[None] * summed
    return (conserved + STEP_SIZE * time_rate, time_rate)
```

```python
import functools

import jax
import jax.numpy as jnp
from jax import lax
from jax.experimental import pallas as pl
from jax.experimental.pallas import tpu as pltpu
from jax.sharding import PartitionSpec as P

GAMMA = 1.4
WENO_EPS = 1e-06
STEP_SIZE = 0.08
MESH = pl.DeviceIdType.MESH
F32 = jnp.float32

Z_DOWN, Z_UP, Y_DOWN, Y_UP, MIRROR, X_DOWN, X_UP, N_SEMS = 0, 3, 6, 9, 12, 15, 16, 17


def recip(value):
    return 1.0 / value


def dot3(first, second):
    return first[0] * second[0] + first[1] * second[1] + first[2] * second[2]


def cell_terms(flow, row):
    density, momentum, energy = flow[0], flow[1:4], flow[4]
    inverse = recip(density)
    velocity = [part * inverse for part in momentum]
    pressure = (GAMMA - 1.0) * energy - (0.5 * (GAMMA - 1.0)) * dot3(momentum, velocity)
    contra = dot3(row, velocity)
    flux = [density * contra]
    flux += [momentum[j] * contra + row[j] * pressure for j in range(3)]
    flux += [(energy + pressure) * contra]
    squared = (GAMMA * pressure * inverse) * dot3(row, row)
    speed = jnp.abs(contra) + squared * lax.rsqrt(squared)
    return velocity, pressure, flux, speed


def weno_part(d0, d1, d2, d3):
    x0, x1, x2 = d1 - d0, d2 - d1, d3 - d2
    e1, e2 = 0.75 * d1, 0.75 * d2
    eps = 3.0 * WENO_EPS
    b0 = (x0 * x0 + eps) + e1 * (x0 + d1)
    b1 = (x1 * x1 + eps) + e1 * d2
    b2 = (x2 * x2 + eps) + e2 * (d2 - x2)
    t12, t02, t01 = b1 * b2, b0 * b2, b0 * b1
    s12, s02, s01 = t12 * t12, t02 * t02, t01 * t01
    w2 = 1.5 * s01
    total = (s12 + 6.0 * s02) + (w2 + w2)
    top = s12 * (x0 - x1) + w2 * (x1 - x2)
    return top * recip(total)


def face_flux(d_flow, d_flux, flux_low, alpha, state, row, sweep):
    e, a, b = (sweep + 1) % 3, (sweep + 2) % 3, sweep
    density, velocity, pressure = state
    inverse_density = recip(density)
    sound2 = GAMMA * pressure * inverse_density
    inverse_sound = lax.rsqrt(sound2)
    sound = sound2 * inverse_sound
    inverse_size = lax.rsqrt(dot3(row, row))
    normal = [row[j] * inverse_size for j in range(3)]
    cross_size = lax.rsqrt(row[a] * row[a] + row[b] * row[b])
    l_a, l_b = row[b] * cross_size, -(row[a] * cross_size)
    m_e = normal[a] * l_b - normal[b] * l_a
    m_a = -(normal[e] * l_b)
    m_b = normal[e] * l_a
    kinetic = 0.5 * dot3(velocity, velocity)
    half_factor = (0.5 * (GAMMA - 1.0)) * inverse_sound * inverse_sound
    half_normal = [(0.5 * inverse_sound) * normal[j] for j in range(3)]

    def project(vector):
        rho = vector[0]
        w = [vector[1 + j] - velocity[j] * rho for j in range(3)]
        half_a = half_factor * ((vector[4] - kinetic * rho) - dot3(velocity, w))
        half_n = dot3(half_normal, w)
        return [
            half_a - half_n,
            rho - (half_a + half_a),
            l_a * w[a] + l_b * w[b],
            m_e * w[e] + m_a * w[a] + m_b * w[b],
            half_a + half_n,
        ]

    scaled = [[alpha * d_flow(m, c) for c in range(5)] for m in range(5)]
    ups = [[scaled[m][c] + d_flux(m, c) for c in range(5)] for m in range(4)]
    downs = [[scaled[m][c] - d_flux(m, c) for c in range(5)] for m in range(1, 5)]
    up_chars = [project(vector) for vector in ups]
    down_chars = [project(vector) for vector in downs]
    chars = [
        weno_part(*[up_chars[m][r] for m in range(4)])
        + weno_part(*[down_chars[m][r] for m in (3, 2, 1, 0)])
        for r in range(5)
    ]
    both = chars[0] + chars[4]
    carried = sound * (chars[4] - chars[0])
    mass = both + chars[1]
    enthalpy = sound2 * (1.0 / (GAMMA - 1.0)) + kinetic
    tangent_speed = l_a * velocity[a] + l_b * velocity[b]
    binormal_speed = m_e * velocity[e] + m_a * velocity[a] + m_b * velocity[b]
    right = [None] * 5
    right[0] = mass
    right[1 + e] = velocity[e] * mass + normal[e] * carried + m_e * chars[3]
    right[1 + a] = (velocity[a] * mass + normal[a] * carried) + (l_a * chars[2] + m_a * chars[3])
    right[1 + b] = (velocity[b] * mass + normal[b] * carried) + (l_b * chars[2] + m_b * chars[3])
    right[4] = (enthalpy * both + kinetic * chars[1]) + (
        (tangent_speed * chars[2] + binormal_speed * chars[3]) + dot3(normal, velocity) * carried
    )
    return [
        (flux_low[c] + 0.5 * d_flux(2, c))
        + (1.0 / 6.0) * ((0.5 * (ups[1][c] + downs[2][c]) - scaled[2][c]) + right[c])
        for c in range(5)
    ]


def line_sweep(cells, terms, faces, sweep, width):
    def prepare(k, _):
        flow = [cells[c, k] for c in range(5)]
        row = [cells[5 + j, k] for j in range(3)]
        velocity, pressure, flux, speed = cell_terms(flow, row)
        for c in range(5):
            terms[c, k] = flux[c]
        terms[5, k] = speed
        for j in range(3):
            terms[6 + j, k] = velocity[j]
        terms[9, k] = pressure
        return _

    lax.fori_loop(0, width + 6, prepare, 0)

    def one_face(k, _):
        alpha = terms[5, k]
        for m in range(1, 6):
            alpha = jnp.maximum(alpha, terms[5, k + m])
        density = 0.5 * (cells[0, k + 2] + cells[0, k + 3])
        velocity = [0.5 * (terms[6 + j, k + 2] + terms[6 + j, k + 3]) for j in range(3)]
        pressure = 0.5 * (terms[9, k + 2] + terms[9, k + 3])
        row = [0.5 * (cells[5 + j, k + 2] + cells[5 + j, k + 3]) for j in range(3)]
        flux = face_flux(
            lambda m, c: cells[c, k + m + 1] - cells[c, k + m],
            lambda m, c: terms[c, k + m + 1] - terms[c, k + m],
            [terms[c, k + 2] for c in range(5)],
            alpha,
            (density, velocity, pressure),
            row,
            sweep,
        )
        for c in range(5):
            faces[c, k] = flux[c]
        return _

    lax.fori_loop(0, width + 1, one_face, 0)


def lane_sweep(flow, row, sweep):
    lanes = flow[0].shape[-1]

    def ahead(value, shift):
        return pltpu.roll(value, (-shift) % lanes, 1)

    velocity, pressure, flux, speed = cell_terms(flow, row)
    pair = jnp.maximum(speed, ahead(speed, 1))
    alpha = jnp.maximum(jnp.maximum(pair, ahead(pair, -2)), ahead(pair, 2))
    mean = lambda value: 0.5 * (value + ahead(value, 1))
    state = (mean(flow[0]), [mean(part) for part in velocity], mean(pressure))
    row_mean = [mean(part) for part in row]
    d_flow = [ahead(part, 1) - part for part in flow]
    d_flux = [ahead(part, 1) - part for part in flux]
    shifted_flow = [[part if m == 2 else ahead(part, m - 2) for part in d_flow] for m in range(5)]
    shifted_flux = [[part if m == 2 else ahead(part, m - 2) for part in d_flux] for m in range(5)]
    return face_flux(
        lambda m, c: shifted_flow[m][c],
        lambda m, c: shifted_flux[m][c],
        flux,
        alpha,
        state,
        row_mean,
        sweep,
    )


def swap_blocks(values, sublane):
    def exchange(first, second, step):
        high = (sublane // step) % 2 == 1
        return (
            jnp.where(high, pltpu.roll(second, step, 0), first),
            jnp.where(high, second, pltpu.roll(first, 8 - step, 0)),
        )

    v0, v1, v2, v3 = values
    v0, v2 = exchange(v0, v2, 2)
    v1, v3 = exchange(v1, v3, 2)
    v0, v1 = exchange(v0, v1, 1)
    v2, v3 = exchange(v2, v3, 1)
    return [v0, v1, v2, v3]


def kernel(
    shape,
    flow_ref,
    metrics_ref,
    wake_ref,
    out_ref,
    zv,
    ym,
    xm,
    wake,
    yv,
    mirror,
    edge,
    edge_low,
    edge_high,
    terms,
    faces,
    x_faces,
    load_sem,
    send_sem,
    recv_sem,
):
    nx, ny, nz = shape
    planes, rows, lanes = flow_ref.shape[1:]
    ix, iy, iz = lax.axis_index("gx"), lax.axis_index("gy"), lax.axis_index("gz")
    partner = nx - 1 - ix
    has_left, has_right = ix > 0, ix < nx - 1
    at_wall, at_top = iy == 0, iy == ny - 1
    z_low = {"gz": lax.rem(iz + nz - 1, nz)}
    z_high = {"gz": lax.rem(iz + 1, nz)}

    barrier = pltpu.get_barrier_semaphore()

    def greet(target):
        pl.semaphore_signal(barrier, inc=1, device_id=target, device_id_type=MESH)

    greet(z_low)
    greet(z_high)
    expected = 2

    @pl.when(has_left)
    def _():
        greet({"gx": ix - 1})

    @pl.when(has_right)
    def _():
        greet({"gx": ix + 1})

    @pl.when(at_wall)
    def _():
        greet({"gx": partner})

    @pl.when(jnp.logical_not(at_wall))
    def _():
        greet({"gy": iy - 1})

    @pl.when(jnp.logical_not(at_top))
    def _():
        greet({"gy": iy + 1})

    own_z = zv.at[:, 3 : 3 + planes]
    loads = [
        pltpu.make_async_copy(flow_ref, zv.at[0:5, 3 : 3 + planes], load_sem.at[0]),
        pltpu.make_async_copy(metrics_ref.at[6:9], zv.at[5:8, 3 : 3 + planes], load_sem.at[1]),
        pltpu.make_async_copy(metrics_ref.at[0:3], xm, load_sem.at[2]),
        pltpu.make_async_copy(metrics_ref.at[3:6], ym, load_sem.at[3]),
        pltpu.make_async_copy(wake_ref, wake, load_sem.at[4]),
    ]
    for copy in loads:
        copy.start()
    for copy in loads:
        copy.wait()

    lane = lax.broadcasted_iota(jnp.int32, (rows, lanes), 1)
    sublane = lax.broadcasted_iota(jnp.int32, (rows, lanes), 0)

    def source(c, p):
        return zv[c, 3 + p] if c < 5 else xm[c - 5, p]

    for c in range(8):
        packed = source(c, planes - 1)
        for p in range(planes):
            value = source(c, p)
            low = pltpu.roll(value, 16 * p + 3, 1)
            high = pltpu.roll(value, (16 * p + 13) % lanes, 1)
            packed = jnp.where((lane >= 16 * p + 3) & (lane < 16 * p + 8), low, packed)
            packed = jnp.where((lane >= 16 * p + 8) & (lane < 16 * p + 13), high, packed)
        edge[c] = packed

    expected = (
        3
        + has_left.astype(jnp.int32)
        + has_right.astype(jnp.int32)
        + jnp.logical_not(at_top).astype(jnp.int32)
    )
    pl.semaphore_wait(barrier, expected)

    def remote(src, dst, index, target):
        return pltpu.make_async_remote_copy(
            src_ref=src,
            dst_ref=dst,
            send_sem=send_sem.at[index],
            recv_sem=recv_sem.at[index],
            device_id=target,
            device_id_type=MESH,
        )

    z_copies = []
    for j in range(3):
        z_copies.append(remote(zv.at[:, 3 + j], zv.at[:, 3 + planes + j], Z_DOWN + j, z_low))
        z_copies.append(
            remote(zv.at[:, 2 + planes - j], zv.at[:, 2 - j], Z_UP + j, z_high)
        )
    for copy in z_copies:
        copy.start()

    x_down = remote(edge, edge_high, X_DOWN, {"gx": ix - 1})
    x_up = remote(edge, edge_low, X_UP, {"gx": ix + 1})

    @pl.when(has_left)
    def _():
        x_down.start()

    @pl.when(has_right)
    def _():
        x_up.start()

    def y_copies(kind):
        copies = []
        for j in range(3):
            if kind == "down":
                index, target, cell = Y_DOWN + j, {"gy": iy - 1}, j
                flow_dst = lambda lo, hi: yv.at[lo:hi, 7 + j, 4:8, :]
            elif kind == "up":
                index, target, cell = Y_UP + j, {"gy": iy + 1}, rows - 3 + j
                flow_dst = lambda lo, hi: yv.at[lo:hi, j, 0:4, :]
            else:
                index, target, cell = MIRROR + j, {"gx": partner}, j
                flow_dst = lambda lo, hi: mirror.at[lo:hi, j, 0:4, :]
            copies.append(
                pltpu.make_async_remote_copy(
                    src_ref=zv.at[0:5, 3 : 3 + planes, cell, :],
                    dst_ref=flow_dst(0, 5),
                    send_sem=send_sem.at[index],
                    recv_sem=recv_sem.at[index],
                    device_id=target,
                    device_id_type=MESH,
                )
            )
            copies.append(
                pltpu.make_async_remote_copy(
                    src_ref=ym.at[:, :, cell, :],
                    dst_ref=flow_dst(5, 8),
                    send_sem=send_sem.at[N_SEMS + index],
                    recv_sem=recv_sem.at[N_SEMS + index],
                    device_id=target,
                    device_id_type=MESH,
                )
            )
        return copies

    y_down, y_up, to_mirror = y_copies("down"), y_copies("up"), y_copies("mirror")

    @pl.when(at_wall)
    def _():
        for copy in to_mirror:
            copy.start()

    @pl.when(jnp.logical_not(at_wall))
    def _():
        for copy in y_down:
            copy.start()

    @pl.when(jnp.logical_not(at_top))
    def _():
        for copy in y_up:
            copy.start()

    def x_plane(p, _):
        flux = lane_sweep([zv[c, 3 + p] for c in range(5)], [xm[j, p] for j in range(3)], 0)
        for c in range(5):
            x_faces[c, p] = flux[c]
        return _

    lax.fori_loop(0, planes, x_plane, 0)

    lower_half = sublane < 4
    for c in range(8):
        swapped = swap_blocks(
            [zv[c, 3 + p] if c < 5 else ym[c - 5, p] for p in range(planes)], sublane
        )
        for k in range(4):
            yv[c, 3 + k] = swapped[k]
        for k in range(3):
            yv[c, k, 4:8] = swapped[1 + k][0:4]
            yv[c, 7 + k, 0:4] = swapped[k][4:8]

    @pl.when(jnp.logical_not(at_top))
    def _():
        for copy in y_down:
            copy.wait_recv()

    @pl.when(at_top)
    def _():
        for c in range(8):
            for k in range(3):
                yv[c, 7 + k, 4:8] = yv[c, 6, 4:8]

    @pl.when(jnp.logical_not(at_wall))
    def _():
        for copy in y_up:
            copy.wait_recv()

    @pl.when(at_wall)
    def _():
        for copy in to_mirror:
            copy.wait_recv()
        is_wake = jnp.broadcast_to(wake[...], (rows, lanes)) >= 0
        backwards = (lanes - 1) - lane
        for c in range(8):
            for k in range(3):
                facing = jnp.take_along_axis(
                    mirror[c, k], backwards, axis=1, mode="promise_in_bounds"
                )
                here = yv[c, 3 + k]
                if 1 <= c <= 3:
                    here = -here
                yv[c, 2 - k, 0:4] = jnp.where(is_wake, facing, here)[0:4]

    line_sweep(yv, terms, faces, 1, 4)
    y_parts = []
    for c in range(5):
        y_parts.append(
            swap_blocks([faces[c, k + 1] - faces[c, k] for k in range(4)], sublane)
        )
    for c in range(5):
        for p in range(planes):
            out_ref[c, p] = y_parts[c][p]

    @pl.when(has_left)
    def _():
        x_up.wait_recv()

    @pl.when(jnp.logical_not(has_left))
    def _():
        for c in range(8):
            for k in range(3):
                moved = pltpu.roll(edge[c], 7 + k, 1)
                edge_low[c] = moved if k == 0 else jnp.where(lane % 16 == 10 + k, moved, edge_low[c])

    @pl.when(has_right)
    def _():
        x_down.wait_recv()

    @pl.when(jnp.logical_not(has_right))
    def _():
        for c in range(8):
            for k in range(3):
                moved = pltpu.roll(edge[c], (3 + k - 12) % lanes, 1)
                edge_high[c] = moved if k == 0 else jnp.where(lane % 16 == 3 + k, moved, edge_high[c])

    place = lane % 16
    ends = []
    for c in range(8):
        value = jnp.where(place < 3, pltpu.roll(edge_low[c], lanes - 10, 1), edge[c])
        value = jnp.where(place >= 13, pltpu.roll(edge_high[c], 10, 1), value)
        ends.append(value)
    ends = lane_sweep(ends[0:5], ends[5:8], 0)
    for c in range(5):
        for p in range(planes):
            low = pltpu.roll(ends[c], (-(16 * p + 3)) % lanes, 1)
            high = pltpu.roll(ends[c], (lanes - 3 - (16 * p + 10)) % lanes, 1)
            upper = jnp.where(lane < 2, low, jnp.where(lane >= lanes - 3, high, x_faces[c, p]))
            lower = pltpu.roll(jnp.where(lane == lanes - 1, low, upper), 1, 1)
            out_ref[c, p] = out_ref[c, p] + (upper - lower)

    for copy in z_copies:
        copy.wait_recv()
    line_sweep(zv, terms, faces, 2, planes)
    for c in range(5):
        for p in range(planes):
            out_ref[c, p] = out_ref[c, p] + (faces[c, p + 1] - faces[c, p])

    for copy in z_copies:
        copy.wait_send()

    @pl.when(has_left)
    def _():
        x_down.wait_send()

    @pl.when(has_right)
    def _():
        x_up.wait_send()

    @pl.when(at_wall)
    def _():
        for copy in to_mirror:
            copy.wait_send()

    @pl.when(jnp.logical_not(at_wall))
    def _():
        for copy in y_down:
            copy.wait_send()

    @pl.when(jnp.logical_not(at_top))
    def _():
        for copy in y_up:
            copy.wait_send()


def solution(mesh):
    nx, ny, nz = mesh.shape["gx"], mesh.shape["gy"], mesh.shape["gz"]

    def local(conserved, metrics, inv_volume, wake_donor):
        planes, rows, lanes = conserved.shape[1:]
        tile = (rows, lanes)
        summed = pl.pallas_call(
            functools.partial(kernel, (nx, ny, nz)),
            out_shape=jax.ShapeDtypeStruct(conserved.shape, F32),
            in_specs=[pl.BlockSpec(memory_space=pl.ANY)] * 3,
            out_specs=pl.BlockSpec(memory_space=pltpu.VMEM),
            scratch_shapes=[
                pltpu.VMEM((8, planes + 6) + tile, F32),
                pltpu.VMEM((3, planes) + tile, F32),
                pltpu.VMEM((3, planes) + tile, F32),
                pltpu.VMEM((1, lanes), jnp.int32),
                pltpu.VMEM((8, 10) + tile, F32),
                pltpu.VMEM((8, 3) + tile, F32),
                pltpu.VMEM((8,) + tile, F32),
                pltpu.VMEM((8,) + tile, F32),
                pltpu.VMEM((8,) + tile, F32),
                pltpu.VMEM((10, 10) + tile, F32),
                pltpu.VMEM((5, 5) + tile, F32),
                pltpu.VMEM((5, planes) + tile, F32),
                pltpu.SemaphoreType.DMA((5,)),
                pltpu.SemaphoreType.DMA((2 * N_SEMS,)),
                pltpu.SemaphoreType.DMA((2 * N_SEMS,)),
            ],
            compiler_params=pltpu.CompilerParams(collective_id=0, has_side_effects=True),
            cost_estimate=pl.CostEstimate(
                flops=60_000_000, bytes_accessed=500_000, transcendentals=0
            ),
        )(conserved, metrics, wake_donor.reshape(1, lanes))
        time_rate = -inv_volume[None] * summed
        return (conserved + STEP_SIZE * time_rate, time_rate)

    placed = (P(None, "gz", "gy", "gx"), P(None, "gz", "gy", "gx"), P("gz", "gy", "gx"), P("gx"))
    return jax.shard_map(
        local,
        mesh=mesh,
        in_specs=placed,
        out_specs=(P(None, "gz", "gy", "gx"), P(None, "gz", "gy", "gx")),
        check_vma=False,
    )
```

```python
import functools

import jax
import jax.numpy as jnp
from jax import lax
from jax.experimental import pallas as pl
from jax.experimental.pallas import tpu as pltpu
from jax.sharding import PartitionSpec as P

GAMMA = 1.4
WENO_EPS = 1e-06
STEP_SIZE = 0.08
MESH = pl.DeviceIdType.MESH
F32 = jnp.float32

Z_DOWN, Z_UP, Y_DOWN, Y_UP, MIRROR, X_DOWN, X_UP, Z_LAST, RELAY, N_SEMS = 0, 3, 6, 9, 12, 15, 16, 17, 18, 21


def recip(value):
    return 1.0 / value


def dot3(first, second):
    return first[0] * second[0] + first[1] * second[1] + first[2] * second[2]


def cell_terms(flow, row):
    density, momentum, energy = flow[0], flow[1:4], flow[4]
    inverse = recip(density)
    velocity = [part * inverse for part in momentum]
    pressure = (GAMMA - 1.0) * energy - (0.5 * (GAMMA - 1.0)) * dot3(momentum, velocity)
    contra = dot3(row, velocity)
    flux = [density * contra]
    flux += [momentum[j] * contra + row[j] * pressure for j in range(3)]
    flux += [(energy + pressure) * contra]
    squared = (GAMMA * pressure * inverse) * dot3(row, row)
    speed = jnp.abs(contra) + squared * lax.rsqrt(squared)
    return velocity, pressure, flux, speed


def weno_part(d0, d1, d2, d3):
    x0, x1, x2 = d1 - d0, d2 - d1, d3 - d2
    e1, e2 = 0.75 * d1, 0.75 * d2
    eps = 3.0 * WENO_EPS
    b0 = (x0 * x0 + eps) + e1 * (x0 + d1)
    b1 = (x1 * x1 + eps) + e1 * d2
    b2 = (x2 * x2 + eps) + e2 * (d2 - x2)
    t12, t02, t01 = b1 * b2, b0 * b2, b0 * b1
    s12, s02, s01 = t12 * t12, t02 * t02, t01 * t01
    w2 = 1.5 * s01
    total = (s12 + 6.0 * s02) + (w2 + w2)
    top = s12 * (x0 - x1) + w2 * (x1 - x2)
    return top * recip(total)


def face_flux(d_flow, d_flux, flux_low, alpha, state, row, sweep):
    e, a, b = (sweep + 1) % 3, (sweep + 2) % 3, sweep
    density, velocity, pressure = state
    inverse_density = recip(density)
    sound2 = GAMMA * pressure * inverse_density
    inverse_sound = lax.rsqrt(sound2)
    sound = sound2 * inverse_sound
    inverse_size = lax.rsqrt(dot3(row, row))
    normal = [row[j] * inverse_size for j in range(3)]
    cross_size = lax.rsqrt(row[a] * row[a] + row[b] * row[b])
    l_a, l_b = row[b] * cross_size, -(row[a] * cross_size)
    m_e = normal[a] * l_b - normal[b] * l_a
    m_a = -(normal[e] * l_b)
    m_b = normal[e] * l_a
    kinetic = 0.5 * dot3(velocity, velocity)
    half_factor = (0.5 * (GAMMA - 1.0)) * inverse_sound * inverse_sound
    half_normal = [(0.5 * inverse_sound) * normal[j] for j in range(3)]

    def project(vector):
        rho = vector[0]
        w = [vector[1 + j] - velocity[j] * rho for j in range(3)]
        half_a = half_factor * ((vector[4] - kinetic * rho) - dot3(velocity, w))
        half_n = dot3(half_normal, w)
        return [
            half_a - half_n,
            rho - (half_a + half_a),
            l_a * w[a] + l_b * w[b],
            m_e * w[e] + m_a * w[a] + m_b * w[b],
            half_a + half_n,
        ]

    scaled = [[alpha * d_flow(m, c) for c in range(5)] for m in range(5)]
    ups = [[scaled[m][c] + d_flux(m, c) for c in range(5)] for m in range(4)]
    downs = [[scaled[m][c] - d_flux(m, c) for c in range(5)] for m in range(1, 5)]
    up_chars = [project(vector) for vector in ups]
    down_chars = [project(vector) for vector in downs]
    chars = [
        weno_part(*[up_chars[m][r] for m in range(4)])
        + weno_part(*[down_chars[m][r] for m in (3, 2, 1, 0)])
        for r in range(5)
    ]
    both = chars[0] + chars[4]
    carried = sound * (chars[4] - chars[0])
    mass = both + chars[1]
    enthalpy = sound2 * (1.0 / (GAMMA - 1.0)) + kinetic
    tangent_speed = l_a * velocity[a] + l_b * velocity[b]
    binormal_speed = m_e * velocity[e] + m_a * velocity[a] + m_b * velocity[b]
    right = [None] * 5
    right[0] = mass
    right[1 + e] = velocity[e] * mass + normal[e] * carried + m_e * chars[3]
    right[1 + a] = (velocity[a] * mass + normal[a] * carried) + (l_a * chars[2] + m_a * chars[3])
    right[1 + b] = (velocity[b] * mass + normal[b] * carried) + (l_b * chars[2] + m_b * chars[3])
    right[4] = (enthalpy * both + kinetic * chars[1]) + (
        (tangent_speed * chars[2] + binormal_speed * chars[3]) + dot3(normal, velocity) * carried
    )
    return [
        (flux_low[c] + 0.5 * d_flux(2, c))
        + (1.0 / 6.0) * ((0.5 * (ups[1][c] + downs[2][c]) - scaled[2][c]) + right[c])
        for c in range(5)
    ]


def line_steps(cells, terms, faces, sweep):
    def prepare(k, _):
        flow = [cells[c, k] for c in range(5)]
        row = [cells[5 + j, k] for j in range(3)]
        velocity, pressure, flux, speed = cell_terms(flow, row)
        for c in range(5):
            terms[c, k] = flux[c]
        terms[5, k] = speed
        for j in range(3):
            terms[6 + j, k] = velocity[j]
        terms[9, k] = pressure
        return _

    def one_face(k, _):
        alpha = terms[5, k]
        for m in range(1, 6):
            alpha = jnp.maximum(alpha, terms[5, k + m])
        density = 0.5 * (cells[0, k + 2] + cells[0, k + 3])
        velocity = [0.5 * (terms[6 + j, k + 2] + terms[6 + j, k + 3]) for j in range(3)]
        pressure = 0.5 * (terms[9, k + 2] + terms[9, k + 3])
        row = [0.5 * (cells[5 + j, k + 2] + cells[5 + j, k + 3]) for j in range(3)]
        flux = face_flux(
            lambda m, c: cells[c, k + m + 1] - cells[c, k + m],
            lambda m, c: terms[c, k + m + 1] - terms[c, k + m],
            [terms[c, k + 2] for c in range(5)],
            alpha,
            (density, velocity, pressure),
            row,
            sweep,
        )
        for c in range(5):
            faces[c, k] = flux[c]
        return _

    return prepare, one_face


def lane_sweep(flow, row, sweep):
    lanes = flow[0].shape[-1]

    def ahead(value, shift):
        return pltpu.roll(value, (-shift) % lanes, 1)

    velocity, pressure, flux, speed = cell_terms(flow, row)
    pair = jnp.maximum(speed, ahead(speed, 1))
    alpha = jnp.maximum(jnp.maximum(pair, ahead(pair, -2)), ahead(pair, 2))
    mean = lambda value: 0.5 * (value + ahead(value, 1))
    state = (mean(flow[0]), [mean(part) for part in velocity], mean(pressure))
    row_mean = [mean(part) for part in row]
    d_flow = [ahead(part, 1) - part for part in flow]
    d_flux = [ahead(part, 1) - part for part in flux]
    shifted_flow = [[part if m == 2 else ahead(part, m - 2) for part in d_flow] for m in range(5)]
    shifted_flux = [[part if m == 2 else ahead(part, m - 2) for part in d_flux] for m in range(5)]
    return face_flux(
        lambda m, c: shifted_flow[m][c],
        lambda m, c: shifted_flux[m][c],
        flux,
        alpha,
        state,
        row_mean,
        sweep,
    )


def swap_blocks(values, sublane):
    def exchange(first, second, step):
        high = (sublane // step) % 2 == 1
        return (
            jnp.where(high, pltpu.roll(second, step, 0), first),
            jnp.where(high, second, pltpu.roll(first, 8 - step, 0)),
        )

    v0, v1, v2, v3 = values
    v0, v2 = exchange(v0, v2, 2)
    v1, v3 = exchange(v1, v3, 2)
    v0, v1 = exchange(v0, v1, 1)
    v2, v3 = exchange(v2, v3, 1)
    return [v0, v1, v2, v3]


def kernel(
    shape,
    flow_ref,
    metrics_ref,
    wake_ref,
    out_ref,
    zv,
    relay,
    ym,
    xm,
    wake,
    yv,
    mirror,
    edge,
    edge_low,
    edge_high,
    terms,
    faces,
    x_faces,
    ready,
    load_sem,
    send_sem,
    recv_sem,
):
    nx, ny, nz = shape
    planes, rows, lanes = flow_ref.shape[1:]
    ix, iy, iz = lax.axis_index("gx"), lax.axis_index("gy"), lax.axis_index("gz")
    partner = nx - 1 - ix
    has_left, has_right = ix > 0, ix < nx - 1
    at_wall, at_top = iy == 0, iy == ny - 1
    z_low = {"gz": lax.rem(iz + nz - 1, nz)}
    z_high = {"gz": lax.rem(iz + 1, nz)}

    barrier = pltpu.get_barrier_semaphore()

    def greet(target):
        pl.semaphore_signal(barrier, inc=1, device_id=target, device_id_type=MESH)

    is_first, is_second, is_last = iz == 0, iz == 1, iz == nz - 1
    mirror_up = at_wall & (partner > ix)
    mirror_down = at_wall & (partner < ix)
    not_first, not_last = jnp.logical_not(is_first), jnp.logical_not(is_last)
    not_wall, not_top = jnp.logical_not(at_wall), jnp.logical_not(at_top)
    x_low, x_high = {"gx": ix - 1}, {"gx": ix + 1}
    y_low, y_high = {"gy": iy - 1}, {"gy": iy + 1}
    opposite = {"gx": partner}

    def when(condition, action):
        pl.when(condition)(action)

    when(not_last, lambda: greet(z_high))
    when(is_first | is_second, lambda: greet({"gz": nz - 1}))
    when(has_right, lambda: greet(x_high))
    when(not_top, lambda: greet(y_high))
    when(mirror_up, lambda: greet(opposite))
    other_core = lax.rem(iy, 2) == 1
    when(other_core, lambda: greet(y_low))

    loads = [
        pltpu.make_async_copy(flow_ref, zv.at[0:5, 3 : 3 + planes], load_sem.at[0]),
        pltpu.make_async_copy(metrics_ref.at[6:9], zv.at[5:8, 3 : 3 + planes], load_sem.at[1]),
        pltpu.make_async_copy(metrics_ref.at[0:3], xm, load_sem.at[2]),
        pltpu.make_async_copy(metrics_ref.at[3:6], ym, load_sem.at[3]),
        pltpu.make_async_copy(wake_ref, wake, load_sem.at[4]),
    ]
    for copy in loads:
        copy.start()
    as_int = lambda flag: flag.astype(jnp.int32)
    pl.semaphore_wait(
        barrier,
        as_int(not_first)
        + 2 * as_int(is_last)
        + as_int(has_left)
        + as_int(not_wall)
        + as_int(mirror_down)
        + as_int(not_top & jnp.logical_not(other_core)),
    )

    def tell(index, target):
        pl.semaphore_signal(ready.at[index], inc=1, device_id=target, device_id_type=MESH)

    def hear(index):
        pl.semaphore_wait(ready.at[index], 1)

    when(not_first, lambda: tell(0, z_low))
    when(is_last, lambda: tell(1, {"gz": 1}))
    when(has_left, lambda: tell(2, x_low))
    when(not_wall, lambda: tell(3, y_low))
    when(mirror_down, lambda: tell(4, opposite))

    lane = lax.broadcasted_iota(jnp.int32, (rows, lanes), 1)
    sublane = lax.broadcasted_iota(jnp.int32, (rows, lanes), 0)

    def remote(src, dst, index, target):
        return pltpu.make_async_remote_copy(
            src_ref=src,
            dst_ref=dst,
            send_sem=send_sem.at[index],
            recv_sem=recv_sem.at[index],
            device_id=target,
            device_id_type=MESH,
        )

    def up_copy(j):
        return remote(zv.at[:, 2 + planes - j], zv.at[:, 2 - j], Z_UP + j, z_high)

    def down_copy(j):
        return remote(zv.at[:, 3 + j], zv.at[:, 3 + planes + j], Z_DOWN + j, z_low)

    def relay_copy(j):
        return pltpu.make_async_remote_copy(
            src_ref=relay if j == 0 else zv.at[:, j - 1],
            dst_ref=zv.at[:, 3 + planes + j],
            send_sem=send_sem.at[RELAY + j],
            recv_sem=recv_sem.at[Z_DOWN + j],
            device_id={"gz": nz - 1},
            device_id_type=MESH,
        )

    extra = remote(zv.at[:, 3], relay, Z_LAST, z_high)
    ups = [up_copy(j) for j in range(3)]
    downs = [down_copy(j) for j in range(3)]
    relays = [relay_copy(j) for j in range(3)]

    def start(copies):
        def action():
            for copy in copies:
                copy.start()

        return action

    for copy in loads[0:2]:
        copy.wait()
    when(is_last & jnp.logical_not(other_core), start(ups))
    when(not_first & not_last, start(downs))
    for copy in loads[2:]:
        copy.wait()

    def source(c, p):
        return zv[c, 3 + p] if c < 5 else xm[c - 5, p]

    for c in range(8):
        packed = source(c, planes - 1)
        for p in range(planes):
            value = source(c, p)
            low = pltpu.roll(value, 16 * p + 3, 1)
            high = pltpu.roll(value, (16 * p + 13) % lanes, 1)
            packed = jnp.where((lane >= 16 * p + 3) & (lane < 16 * p + 8), low, packed)
            packed = jnp.where((lane >= 16 * p + 8) & (lane < 16 * p + 13), high, packed)
        edge[c] = packed

    x_down = remote(edge, edge_high, X_DOWN, x_low)
    x_up = remote(edge, edge_low, X_UP, x_high)
    when(has_left, x_down.start)

    def y_copies(kind):
        copies = []
        for j in range(3):
            if kind == "down":
                index, target, cell = Y_DOWN + j, {"gy": iy - 1}, j
                flow_dst = lambda lo, hi: yv.at[lo:hi, 7 + j, 4:8, :]
            elif kind == "up":
                index, target, cell = Y_UP + j, {"gy": iy + 1}, rows - 3 + j
                flow_dst = lambda lo, hi: yv.at[lo:hi, j, 0:4, :]
            else:
                index, target, cell = MIRROR + j, {"gx": partner}, j
                flow_dst = lambda lo, hi: mirror.at[lo:hi, j, 0:4, :]
            copies.append(
                pltpu.make_async_remote_copy(
                    src_ref=zv.at[0:5, 3 : 3 + planes, cell, :],
                    dst_ref=flow_dst(0, 5),
                    send_sem=send_sem.at[index],
                    recv_sem=recv_sem.at[index],
                    device_id=target,
                    device_id_type=MESH,
                )
            )
            copies.append(
                pltpu.make_async_remote_copy(
                    src_ref=ym.at[:, :, cell, :],
                    dst_ref=flow_dst(5, 8),
                    send_sem=send_sem.at[N_SEMS + index],
                    recv_sem=recv_sem.at[N_SEMS + index],
                    device_id=target,
                    device_id_type=MESH,
                )
            )
        return copies

    y_down, y_up, to_mirror = y_copies("down"), y_copies("up"), y_copies("mirror")

    when(not_wall, start(y_down))
    when(mirror_down, start(to_mirror))

    def x_plane(p, _):
        flux = lane_sweep([zv[c, 3 + p] for c in range(5)], [xm[j, p] for j in range(3)], 0)
        for c in range(5):
            x_faces[c, p] = flux[c]
        return _

    lax.fori_loop(0, planes, x_plane, 0)

    when(is_last & other_core, start(ups))

    @pl.when(not_last)
    def _():
        hear(0)
        when(is_first, extra.start)
        start([ups[2], ups[1], ups[0]])()

    @pl.when(mirror_up)
    def _():
        hear(4)
        start(to_mirror)()

    @pl.when(not_top)
    def _():
        hear(3)
        start(y_up)()

    @pl.when(has_right)
    def _():
        hear(2)
        x_up.start()

    @pl.when(is_second)
    def _():
        extra.wait_recv()
        for copy in ups:
            copy.wait_recv()
        hear(1)
        start(relays)()

    when(is_last, start(downs))

    lower_half = sublane < 4
    for c in range(8):
        swapped = swap_blocks(
            [zv[c, 3 + p] if c < 5 else ym[c - 5, p] for p in range(planes)], sublane
        )
        for k in range(4):
            yv[c, 3 + k] = swapped[k]
        for k in range(3):
            yv[c, k, 4:8] = swapped[1 + k][0:4]
            yv[c, 7 + k, 0:4] = swapped[k][4:8]

    @pl.when(jnp.logical_not(at_top))
    def _():
        for copy in y_down:
            copy.wait_recv()

    @pl.when(at_top)
    def _():
        for c in range(8):
            for k in range(3):
                yv[c, 7 + k, 4:8] = yv[c, 6, 4:8]

    @pl.when(jnp.logical_not(at_wall))
    def _():
        for copy in y_up:
            copy.wait_recv()

    @pl.when(at_wall)
    def _():
        for copy in to_mirror:
            copy.wait_recv()
        is_wake = jnp.broadcast_to(wake[...], (rows, lanes)) >= 0
        backwards = (lanes - 1) - lane
        for c in range(8):
            for k in range(3):
                facing = jnp.take_along_axis(
                    mirror[c, k], backwards, axis=1, mode="promise_in_bounds"
                )
                here = yv[c, 3 + k]
                if 1 <= c <= 3:
                    here = -here
                yv[c, 2 - k, 0:4] = jnp.where(is_wake, facing, here)[0:4]

    prepare, one_face = line_steps(yv, terms, faces, 1)
    lax.fori_loop(0, 10, prepare, 0)
    lax.fori_loop(0, 5, one_face, 0)
    y_parts = []
    for c in range(5):
        y_parts.append(
            swap_blocks([faces[c, k] - faces[c, k + 1] for k in range(4)], sublane)
        )
    for c in range(5):
        for p in range(planes):
            out_ref[c, p] = y_parts[c][p]

    @pl.when(has_left)
    def _():
        x_up.wait_recv()

    @pl.when(jnp.logical_not(has_left))
    def _():
        for c in range(8):
            for k in range(3):
                moved = pltpu.roll(edge[c], 7 + k, 1)
                edge_low[c] = moved if k == 0 else jnp.where(lane % 16 == 10 + k, moved, edge_low[c])

    @pl.when(has_right)
    def _():
        x_down.wait_recv()

    @pl.when(jnp.logical_not(has_right))
    def _():
        for c in range(8):
            for k in range(3):
                moved = pltpu.roll(edge[c], (3 + k - 12) % lanes, 1)
                edge_high[c] = moved if k == 0 else jnp.where(lane % 16 == 3 + k, moved, edge_high[c])

    place = lane % 16
    ends = []
    for c in range(8):
        value = jnp.where(place < 3, pltpu.roll(edge_low[c], lanes - 10, 1), edge[c])
        value = jnp.where(place >= 13, pltpu.roll(edge_high[c], 10, 1), value)
        ends.append(value)
    ends = lane_sweep(ends[0:5], ends[5:8], 0)
    for c in range(5):
        for p in range(planes):
            low = pltpu.roll(ends[c], (-(16 * p + 3)) % lanes, 1)
            high = pltpu.roll(ends[c], (lanes - 3 - (16 * p + 10)) % lanes, 1)
            upper = jnp.where(lane < 2, low, jnp.where(lane >= lanes - 3, high, x_faces[c, p]))
            lower = pltpu.roll(jnp.where(lane == lanes - 1, low, upper), 1, 1)
            out_ref[c, p] = out_ref[c, p] + (lower - upper)

    prepare, one_face = line_steps(zv, terms, faces, 2)
    lax.fori_loop(3, 3 + planes, prepare, 0)
    for copy in downs:
        copy.wait_recv()
    lax.fori_loop(3 + planes, 6 + planes, prepare, 0)

    def finish(k, _):
        for c in range(5):
            out_ref[c, k] = out_ref[c, k] + (faces[c, k] - faces[c, k + 1])
        return _

    lax.fori_loop(3, planes + 1, one_face, 0)
    lax.fori_loop(3, planes, finish, 0)

    def near_face(j, carry):
        k = 2 - j

        @pl.when(jnp.logical_not(is_second))
        def _():
            up_copy(j).wait_recv()

        prepare(k, 0)
        one_face(k, 0)
        finish(k, 0)
        return carry

    lax.fori_loop(0, 3, near_face, 0)

    for copy in ups:
        copy.wait_send()

    @pl.when(is_first)
    def _():
        extra.wait_send()

    @pl.when(jnp.logical_not(is_first))
    def _():
        for copy in downs:
            copy.wait_send()

    @pl.when(is_second)
    def _():
        for copy in relays:
            copy.wait_send()

    @pl.when(has_left)
    def _():
        x_down.wait_send()

    @pl.when(has_right)
    def _():
        x_up.wait_send()

    @pl.when(at_wall)
    def _():
        for copy in to_mirror:
            copy.wait_send()

    @pl.when(jnp.logical_not(at_wall))
    def _():
        for copy in y_down:
            copy.wait_send()

    @pl.when(jnp.logical_not(at_top))
    def _():
        for copy in y_up:
            copy.wait_send()


def solution(mesh):
    nx, ny, nz = mesh.shape["gx"], mesh.shape["gy"], mesh.shape["gz"]

    def local(conserved, metrics, inv_volume, wake_donor):
        planes, rows, lanes = conserved.shape[1:]
        tile = (rows, lanes)
        operands = (conserved, metrics, wake_donor.reshape(1, lanes))
        summed = pl.pallas_call(
            functools.partial(kernel, (nx, ny, nz)),
            out_shape=jax.ShapeDtypeStruct(conserved.shape, F32),
            in_specs=[pl.BlockSpec(memory_space=pltpu.HBM)] * 3,
            out_specs=pl.BlockSpec(memory_space=pltpu.VMEM),
            scratch_shapes=[
                pltpu.VMEM((8, planes + 6) + tile, F32),
                pltpu.VMEM((8,) + tile, F32),
                pltpu.VMEM((3, planes) + tile, F32),
                pltpu.VMEM((3, planes) + tile, F32),
                pltpu.VMEM((1, lanes), jnp.int32),
                pltpu.VMEM((8, 10) + tile, F32),
                pltpu.VMEM((8, 3) + tile, F32),
                pltpu.VMEM((8,) + tile, F32),
                pltpu.VMEM((8,) + tile, F32),
                pltpu.VMEM((8,) + tile, F32),
                pltpu.VMEM((10, 10) + tile, F32),
                pltpu.VMEM((5, 5) + tile, F32),
                pltpu.VMEM((5, planes) + tile, F32),
                pltpu.SemaphoreType.REGULAR((5,)),
                pltpu.SemaphoreType.DMA((5,)),
                pltpu.SemaphoreType.DMA((2 * N_SEMS,)),
                pltpu.SemaphoreType.DMA((2 * N_SEMS,)),
            ],
            compiler_params=pltpu.CompilerParams(
                collective_id=0, has_side_effects=True, vmem_limit_bytes=8 * 1024 * 1024
            ),
            cost_estimate=pl.CostEstimate(
                flops=60_000_000, bytes_accessed=500_000, transcendentals=0
            ),
        )(*[pltpu.with_memory_space_constraint(x, pltpu.HBM) for x in operands])
        time_rate = inv_volume[None] * summed
        return (conserved + STEP_SIZE * time_rate, time_rate)

    placed = (P(None, "gz", "gy", "gx"), P(None, "gz", "gy", "gx"), P("gz", "gy", "gx"), P("gx"))
    return jax.shard_map(
        local,
        mesh=mesh,
        in_specs=placed,
        out_specs=(P(None, "gz", "gy", "gx"), P(None, "gz", "gy", "gx")),
        check_vma=False,
    )
```

```python
import functools

import jax
import jax.numpy as jnp
from jax import lax
from jax.experimental import pallas as pl
from jax.experimental.pallas import tpu as pltpu
from jax.sharding import PartitionSpec as P

GAMMA = 1.4
WENO_EPS = 1e-06
STEP_SIZE = 0.08
MESH = pl.DeviceIdType.MESH
F32 = jnp.float32

Z_DOWN, Z_UP, Y_DOWN, Y_UP, MIRROR, X_DOWN, X_UP, Z_LAST, RELAY, N_SEMS = 0, 3, 6, 9, 12, 15, 16, 17, 18, 21


def recip(value):
    return 1.0 / value


def dot3(first, second):
    return first[0] * second[0] + first[1] * second[1] + first[2] * second[2]


def cell_terms(flow, row):
    density, momentum, energy = flow[0], flow[1:4], flow[4]
    inverse = recip(density)
    velocity = [part * inverse for part in momentum]
    pressure = (GAMMA - 1.0) * energy - (0.5 * (GAMMA - 1.0)) * dot3(momentum, velocity)
    contra = dot3(row, velocity)
    flux = [density * contra]
    flux += [momentum[j] * contra + row[j] * pressure for j in range(3)]
    flux += [(energy + pressure) * contra]
    squared = (GAMMA * pressure * inverse) * dot3(row, row)
    speed = jnp.abs(contra) + squared * lax.rsqrt(squared)
    return velocity, pressure, flux, speed


def weno_part(d0, d1, d2, d3):
    x0, x1, x2 = d1 - d0, d2 - d1, d3 - d2
    e1, e2 = 0.75 * d1, 0.75 * d2
    eps = 3.0 * WENO_EPS
    b0 = (x0 * x0 + eps) + e1 * (x0 + d1)
    b1 = (x1 * x1 + eps) + e1 * d2
    b2 = (x2 * x2 + eps) + e2 * (d2 - x2)
    t12, t02, t01 = b1 * b2, b0 * b2, b0 * b1
    s12, s02, s01 = t12 * t12, t02 * t02, t01 * t01
    w2 = 1.5 * s01
    total = (s12 + 6.0 * s02) + (w2 + w2)
    top = s12 * (x0 - x1) + w2 * (x1 - x2)
    return top * recip(total)


def face_flux(d_flow, d_flux, flux_low, alpha, state, row, sweep):
    e, a, b = (sweep + 1) % 3, (sweep + 2) % 3, sweep
    density, velocity, pressure = state
    inverse_density = recip(density)
    sound2 = GAMMA * pressure * inverse_density
    inverse_sound = lax.rsqrt(sound2)
    sound = sound2 * inverse_sound
    inverse_size = lax.rsqrt(dot3(row, row))
    normal = [row[j] * inverse_size for j in range(3)]
    cross_size = lax.rsqrt(row[a] * row[a] + row[b] * row[b])
    l_a, l_b = row[b] * cross_size, -(row[a] * cross_size)
    m_e = normal[a] * l_b - normal[b] * l_a
    m_a = -(normal[e] * l_b)
    m_b = normal[e] * l_a
    kinetic = 0.5 * dot3(velocity, velocity)
    half_factor = (0.5 * (GAMMA - 1.0)) * inverse_sound * inverse_sound
    half_normal = [(0.5 * inverse_sound) * normal[j] for j in range(3)]

    def project(vector):
        rho = vector[0]
        w = [vector[1 + j] - velocity[j] * rho for j in range(3)]
        half_a = half_factor * ((vector[4] - kinetic * rho) - dot3(velocity, w))
        half_n = dot3(half_normal, w)
        return [
            half_a - half_n,
            rho - (half_a + half_a),
            l_a * w[a] + l_b * w[b],
            m_e * w[e] + m_a * w[a] + m_b * w[b],
            half_a + half_n,
        ]

    scaled = [[alpha * d_flow(m, c) for c in range(5)] for m in range(5)]
    ups = [[scaled[m][c] + d_flux(m, c) for c in range(5)] for m in range(4)]
    downs = [[scaled[m][c] - d_flux(m, c) for c in range(5)] for m in range(1, 5)]
    up_chars = [project(vector) for vector in ups]
    down_chars = [project(vector) for vector in downs]
    chars = [
        weno_part(*[up_chars[m][r] for m in range(4)])
        + weno_part(*[down_chars[m][r] for m in (3, 2, 1, 0)])
        for r in range(5)
    ]
    both = chars[0] + chars[4]
    carried = sound * (chars[4] - chars[0])
    mass = both + chars[1]
    enthalpy = sound2 * (1.0 / (GAMMA - 1.0)) + kinetic
    tangent_speed = l_a * velocity[a] + l_b * velocity[b]
    binormal_speed = m_e * velocity[e] + m_a * velocity[a] + m_b * velocity[b]
    right = [None] * 5
    right[0] = mass
    right[1 + e] = velocity[e] * mass + normal[e] * carried + m_e * chars[3]
    right[1 + a] = (velocity[a] * mass + normal[a] * carried) + (l_a * chars[2] + m_a * chars[3])
    right[1 + b] = (velocity[b] * mass + normal[b] * carried) + (l_b * chars[2] + m_b * chars[3])
    right[4] = (enthalpy * both + kinetic * chars[1]) + (
        (tangent_speed * chars[2] + binormal_speed * chars[3]) + dot3(normal, velocity) * carried
    )
    return [
        (flux_low[c] + 0.5 * d_flux(2, c))
        + (1.0 / 6.0) * ((0.5 * (ups[1][c] + downs[2][c]) - scaled[2][c]) + right[c])
        for c in range(5)
    ]


def line_steps(cells, terms, faces, sweep):
    def prepare(k, _):
        flow = [cells[c, k] for c in range(5)]
        row = [cells[5 + j, k] for j in range(3)]
        velocity, pressure, flux, speed = cell_terms(flow, row)
        for c in range(5):
            terms[c, k] = flux[c]
        terms[5, k] = speed
        for j in range(3):
            terms[6 + j, k] = velocity[j]
        terms[9, k] = pressure
        return _

    def one_face(k, _):
        alpha = terms[5, k]
        for m in range(1, 6):
            alpha = jnp.maximum(alpha, terms[5, k + m])
        density = 0.5 * (cells[0, k + 2] + cells[0, k + 3])
        velocity = [0.5 * (terms[6 + j, k + 2] + terms[6 + j, k + 3]) for j in range(3)]
        pressure = 0.5 * (terms[9, k + 2] + terms[9, k + 3])
        row = [0.5 * (cells[5 + j, k + 2] + cells[5 + j, k + 3]) for j in range(3)]
        flux = face_flux(
            lambda m, c: cells[c, k + m + 1] - cells[c, k + m],
            lambda m, c: terms[c, k + m + 1] - terms[c, k + m],
            [terms[c, k + 2] for c in range(5)],
            alpha,
            (density, velocity, pressure),
            row,
            sweep,
        )
        for c in range(5):
            faces[c, k] = flux[c]
        return _

    return prepare, one_face


def lane_sweep(flow, row, sweep):
    lanes = flow[0].shape[-1]

    def ahead(value, shift):
        return pltpu.roll(value, (-shift) % lanes, 1)

    velocity, pressure, flux, speed = cell_terms(flow, row)
    pair = jnp.maximum(speed, ahead(speed, 1))
    alpha = jnp.maximum(jnp.maximum(pair, ahead(pair, -2)), ahead(pair, 2))
    mean = lambda value: 0.5 * (value + ahead(value, 1))
    state = (mean(flow[0]), [mean(part) for part in velocity], mean(pressure))
    row_mean = [mean(part) for part in row]
    d_flow = [ahead(part, 1) - part for part in flow]
    d_flux = [ahead(part, 1) - part for part in flux]
    shifted_flow = [[part if m == 2 else ahead(part, m - 2) for part in d_flow] for m in range(5)]
    shifted_flux = [[part if m == 2 else ahead(part, m - 2) for part in d_flux] for m in range(5)]
    return face_flux(
        lambda m, c: shifted_flow[m][c],
        lambda m, c: shifted_flux[m][c],
        flux,
        alpha,
        state,
        row_mean,
        sweep,
    )


def swap_blocks(values, sublane):
    def exchange(first, second, step):
        high = (sublane // step) % 2 == 1
        return (
            jnp.where(high, pltpu.roll(second, step, 0), first),
            jnp.where(high, second, pltpu.roll(first, 8 - step, 0)),
        )

    v0, v1, v2, v3 = values
    v0, v2 = exchange(v0, v2, 2)
    v1, v3 = exchange(v1, v3, 2)
    v0, v1 = exchange(v0, v1, 1)
    v2, v3 = exchange(v2, v3, 1)
    return [v0, v1, v2, v3]


def kernel(
    shape,
    flow_ref,
    metrics_ref,
    inv_ref,
    wake_ref,
    state_ref,
    rate_ref,
    zv,
    relay,
    ym,
    xm,
    wake,
    inv,
    yv,
    mirror,
    edge,
    edge_low,
    edge_high,
    terms,
    faces,
    x_faces,
    ready,
    load_sem,
    send_sem,
    recv_sem,
):
    nx, ny, nz = shape
    planes, rows, lanes = flow_ref.shape[1:]
    ix, iy, iz = lax.axis_index("gx"), lax.axis_index("gy"), lax.axis_index("gz")
    partner = nx - 1 - ix
    has_left, has_right = ix > 0, ix < nx - 1
    at_wall, at_top = iy == 0, iy == ny - 1
    z_low = {"gz": lax.rem(iz + nz - 1, nz)}
    z_high = {"gz": lax.rem(iz + 1, nz)}

    loads = [
        pltpu.make_async_copy(flow_ref, zv.at[0:5, 3 : 3 + planes], load_sem.at[0]),
        pltpu.make_async_copy(metrics_ref.at[6:9], zv.at[5:8, 3 : 3 + planes], load_sem.at[1]),
        pltpu.make_async_copy(metrics_ref.at[0:3], xm, load_sem.at[2]),
        pltpu.make_async_copy(metrics_ref.at[3:6], ym, load_sem.at[3]),
        pltpu.make_async_copy(wake_ref, wake, load_sem.at[4]),
        pltpu.make_async_copy(inv_ref, inv, load_sem.at[5]),
    ]
    for copy in loads:
        copy.start()

    barrier = pltpu.get_barrier_semaphore()

    def greet(target):
        pl.semaphore_signal(barrier, inc=1, device_id=target, device_id_type=MESH)

    is_first, is_second, is_last = iz == 0, iz == 1, iz == nz - 1
    mirror_up = at_wall & (partner > ix)
    mirror_down = at_wall & (partner < ix)
    not_first, not_last = jnp.logical_not(is_first), jnp.logical_not(is_last)
    not_wall, not_top = jnp.logical_not(at_wall), jnp.logical_not(at_top)
    x_low, x_high = {"gx": ix - 1}, {"gx": ix + 1}
    y_low, y_high = {"gy": iy - 1}, {"gy": iy + 1}
    opposite = {"gx": partner}

    def when(condition, action):
        pl.when(condition)(action)

    when(not_last, lambda: greet(z_high))
    when(is_first | is_second, lambda: greet({"gz": nz - 1}))
    when(has_right, lambda: greet(x_high))
    when(not_top, lambda: greet(y_high))
    when(mirror_up, lambda: greet(opposite))
    other_core = lax.rem(iy, 2) == 1
    when(other_core, lambda: greet(y_low))

    for copy in loads[0:2]:
        copy.wait()
    as_int = lambda flag: flag.astype(jnp.int32)
    pl.semaphore_wait(
        barrier,
        as_int(not_first)
        + 2 * as_int(is_last)
        + as_int(has_left)
        + as_int(not_wall)
        + as_int(mirror_down)
        + as_int(not_top & jnp.logical_not(other_core)),
    )

    lane = lax.broadcasted_iota(jnp.int32, (rows, lanes), 1)
    sublane = lax.broadcasted_iota(jnp.int32, (rows, lanes), 0)

    def remote(src, dst, index, target):
        return pltpu.make_async_remote_copy(
            src_ref=src,
            dst_ref=dst,
            send_sem=send_sem.at[index],
            recv_sem=recv_sem.at[index],
            device_id=target,
            device_id_type=MESH,
        )

    def up_copy(j):
        return remote(zv.at[:, 2 + planes - j], zv.at[:, 2 - j], Z_UP + j, z_high)

    def down_copy(j):
        return remote(zv.at[:, 3 + j], zv.at[:, 3 + planes + j], Z_DOWN + j, z_low)

    def relay_copy(j):
        return pltpu.make_async_remote_copy(
            src_ref=relay if j == 0 else zv.at[:, j - 1],
            dst_ref=zv.at[:, 3 + planes + j],
            send_sem=send_sem.at[RELAY + j],
            recv_sem=recv_sem.at[Z_DOWN + j],
            device_id={"gz": nz - 1},
            device_id_type=MESH,
        )

    extra = remote(zv.at[:, 3], relay, Z_LAST, z_high)
    ups = [up_copy(j) for j in range(3)]
    downs = [down_copy(j) for j in range(3)]
    relays = [relay_copy(j) for j in range(3)]

    def start(copies):
        def action():
            for copy in copies:
                copy.start()

        return action

    when(is_last & jnp.logical_not(other_core), start(ups))

    def tell(index, target):
        pl.semaphore_signal(ready.at[index], inc=1, device_id=target, device_id_type=MESH)

    def hear(index):
        pl.semaphore_wait(ready.at[index], 1)

    when(not_first, lambda: tell(0, z_low))
    when(is_last, lambda: tell(1, {"gz": 1}))
    when(has_left, lambda: tell(2, x_low))
    when(not_wall, lambda: tell(3, y_low))
    when(mirror_down, lambda: tell(4, opposite))

    when(not_first & not_last, start(downs))
    for copy in loads[2:]:
        copy.wait()

    def source(c, p):
        return zv[c, 3 + p] if c < 5 else xm[c - 5, p]

    for c in range(8):
        packed = source(c, planes - 1)
        for p in range(planes):
            value = source(c, p)
            low = pltpu.roll(value, 16 * p + 3, 1)
            high = pltpu.roll(value, (16 * p + 13) % lanes, 1)
            packed = jnp.where((lane >= 16 * p + 3) & (lane < 16 * p + 8), low, packed)
            packed = jnp.where((lane >= 16 * p + 8) & (lane < 16 * p + 13), high, packed)
        edge[c] = packed

    x_down = remote(edge, edge_high, X_DOWN, x_low)
    x_up = remote(edge, edge_low, X_UP, x_high)
    when(has_left, x_down.start)

    def y_copies(kind):
        copies = []
        for j in range(3):
            if kind == "down":
                index, target, cell = Y_DOWN + j, {"gy": iy - 1}, j
                flow_dst = lambda lo, hi: yv.at[lo:hi, 7 + j, 4:8, :]
            elif kind == "up":
                index, target, cell = Y_UP + j, {"gy": iy + 1}, rows - 3 + j
                flow_dst = lambda lo, hi: yv.at[lo:hi, j, 0:4, :]
            else:
                index, target, cell = MIRROR + j, {"gx": partner}, j
                flow_dst = lambda lo, hi: mirror.at[lo:hi, j, 0:4, :]
            copies.append(
                pltpu.make_async_remote_copy(
                    src_ref=zv.at[0:5, 3 : 3 + planes, cell, :],
                    dst_ref=flow_dst(0, 5),
                    send_sem=send_sem.at[index],
                    recv_sem=recv_sem.at[index],
                    device_id=target,
                    device_id_type=MESH,
                )
            )
            copies.append(
                pltpu.make_async_remote_copy(
                    src_ref=ym.at[:, :, cell, :],
                    dst_ref=flow_dst(5, 8),
                    send_sem=send_sem.at[N_SEMS + index],
                    recv_sem=recv_sem.at[N_SEMS + index],
                    device_id=target,
                    device_id_type=MESH,
                )
            )
        return copies

    y_down, y_up, to_mirror = y_copies("down"), y_copies("up"), y_copies("mirror")

    when(not_wall, start(y_down))
    when(mirror_down, start(to_mirror))

    @pl.when(not_last)
    def _():
        hear(0)
        when(is_first, extra.start)
        start([ups[2], ups[1], ups[0]])()

    def x_plane(p, _):
        when(is_last & other_core & (p == planes - 1), start(ups))
        flux = lane_sweep([zv[c, 3 + p] for c in range(5)], [xm[j, p] for j in range(3)], 0)
        for c in range(5):
            x_faces[c, p] = flux[c]
        return _

    lax.fori_loop(0, planes, x_plane, 0)

    @pl.when(mirror_up)
    def _():
        hear(4)
        start(to_mirror)()

    @pl.when(not_top)
    def _():
        hear(3)
        start(y_up)()

    @pl.when(has_right)
    def _():
        hear(2)
        x_up.start()

    @pl.when(is_second)
    def _():
        extra.wait_recv()
        ups[2].wait_recv()
        ups[1].wait_recv()
        hear(1)
        start(relays)()

    when(is_last, start(downs))

    lower_half = sublane < 4
    for c in range(8):
        swapped = swap_blocks(
            [zv[c, 3 + p] if c < 5 else ym[c - 5, p] for p in range(planes)], sublane
        )
        for k in range(4):
            yv[c, 3 + k] = swapped[k]
        for k in range(3):
            yv[c, k, 4:8] = swapped[1 + k][0:4]
            yv[c, 7 + k, 0:4] = swapped[k][4:8]

    @pl.when(jnp.logical_not(at_top))
    def _():
        for copy in y_down:
            copy.wait_recv()

    @pl.when(at_top)
    def _():
        for c in range(8):
            for k in range(3):
                yv[c, 7 + k, 4:8] = yv[c, 6, 4:8]

    @pl.when(jnp.logical_not(at_wall))
    def _():
        for copy in y_up:
            copy.wait_recv()

    @pl.when(at_wall)
    def _():
        for copy in to_mirror:
            copy.wait_recv()
        is_wake = jnp.broadcast_to(wake[...], (rows, lanes)) >= 0
        backwards = (lanes - 1) - lane
        for c in range(8):
            for k in range(3):
                facing = jnp.take_along_axis(
                    mirror[c, k], backwards, axis=1, mode="promise_in_bounds"
                )
                here = yv[c, 3 + k]
                if 1 <= c <= 3:
                    here = -here
                yv[c, 2 - k, 0:4] = jnp.where(is_wake, facing, here)[0:4]

    prepare, one_face = line_steps(yv, terms, faces, 1)
    lax.fori_loop(0, 10, prepare, 0)
    lax.fori_loop(0, 5, one_face, 0)
    y_parts = []
    for c in range(5):
        y_parts.append(
            swap_blocks([faces[c, k] - faces[c, k + 1] for k in range(4)], sublane)
        )
    for c in range(5):
        for p in range(planes):
            rate_ref[c, p] = y_parts[c][p]

    @pl.when(has_left)
    def _():
        x_up.wait_recv()

    @pl.when(jnp.logical_not(has_left))
    def _():
        for c in range(8):
            for k in range(3):
                moved = pltpu.roll(edge[c], 7 + k, 1)
                edge_low[c] = moved if k == 0 else jnp.where(lane % 16 == 10 + k, moved, edge_low[c])

    @pl.when(has_right)
    def _():
        x_down.wait_recv()

    @pl.when(jnp.logical_not(has_right))
    def _():
        for c in range(8):
            for k in range(3):
                moved = pltpu.roll(edge[c], (3 + k - 12) % lanes, 1)
                edge_high[c] = moved if k == 0 else jnp.where(lane % 16 == 3 + k, moved, edge_high[c])

    place = lane % 16
    ends = []
    for c in range(8):
        value = jnp.where(place < 3, pltpu.roll(edge_low[c], lanes - 10, 1), edge[c])
        value = jnp.where(place >= 13, pltpu.roll(edge_high[c], 10, 1), value)
        ends.append(value)
    ends = lane_sweep(ends[0:5], ends[5:8], 0)
    for c in range(5):
        for p in range(planes):
            low = pltpu.roll(ends[c], (-(16 * p + 3)) % lanes, 1)
            high = pltpu.roll(ends[c], (lanes - 3 - (16 * p + 10)) % lanes, 1)
            upper = jnp.where(lane < 2, low, jnp.where(lane >= lanes - 3, high, x_faces[c, p]))
            lower = pltpu.roll(jnp.where(lane == lanes - 1, low, upper), 1, 1)
            rate_ref[c, p] = rate_ref[c, p] + (lower - upper)

    prepare, one_face = line_steps(zv, terms, faces, 2)
    lax.fori_loop(3, 3 + planes, prepare, 0)
    below_last = 2 * iz < nz
    pick = lambda low, high: jnp.where(below_last, low, high)

    def arrival(slot, index):
        return remote(zv.at[:, 3], zv.at[:, slot], index, z_high)

    def finish(k, _):
        volume = inv[k]
        for c in range(5):
            rate = volume * (rate_ref[c, k] + (faces[c, k] - faces[c, k + 1]))
            rate_ref[c, k] = rate
            state_ref[c, k] = zv[c, 3 + k] + STEP_SIZE * rate
        return _

    def soon(j, carry):
        slot = pick(7 + j, 2 - j)
        arrival(slot, pick(Z_DOWN + j, Z_UP + j)).wait_recv()
        return prepare(slot, carry)

    lax.fori_loop(0, 3, soon, 0)
    lax.fori_loop(0, 2, lambda j, carry: one_face(pick(3 + j, j), carry), 0)
    finish(pick(3, 0), 0)

    def late(j, carry):
        slot = pick(2 - j, 7 + j)

        @pl.when(jnp.logical_not(is_second) | (j == 0))
        def _():
            arrival(slot, pick(Z_UP + j, Z_DOWN + j)).wait_recv()

        prepare(slot, 0)
        one_face(pick(2 - j, 2 + j), 0)
        finish(pick(2 - j, 1 + j), 0)
        return carry

    lax.fori_loop(0, 3, late, 0)

    for copy in ups:
        copy.wait_send()

    @pl.when(is_first)
    def _():
        extra.wait_send()

    @pl.when(jnp.logical_not(is_first))
    def _():
        for copy in downs:
            copy.wait_send()

    @pl.when(is_second)
    def _():
        for copy in relays:
            copy.wait_send()

    @pl.when(has_left)
    def _():
        x_down.wait_send()

    @pl.when(has_right)
    def _():
        x_up.wait_send()

    @pl.when(at_wall)
    def _():
        for copy in to_mirror:
            copy.wait_send()

    @pl.when(jnp.logical_not(at_wall))
    def _():
        for copy in y_down:
            copy.wait_send()

    @pl.when(jnp.logical_not(at_top))
    def _():
        for copy in y_up:
            copy.wait_send()


def store(state_ref, rate_ref, state_out, rate_out, sem):
    copies = [
        pltpu.make_async_copy(state_ref, state_out, sem.at[0]),
        pltpu.make_async_copy(rate_ref, rate_out, sem.at[1]),
    ]
    for copy in copies:
        copy.start()
    for copy in copies:
        copy.wait()


def solution(mesh):
    nx, ny, nz = mesh.shape["gx"], mesh.shape["gy"], mesh.shape["gz"]

    def local(conserved, metrics, inv_volume, wake_donor):
        planes, rows, lanes = conserved.shape[1:]
        tile = (rows, lanes)
        operands = (conserved, metrics, inv_volume, wake_donor.reshape(1, lanes))
        results = pl.pallas_call(
            functools.partial(kernel, (nx, ny, nz)),
            out_shape=[jax.ShapeDtypeStruct(conserved.shape, F32)] * 2,
            in_specs=[pl.BlockSpec(memory_space=pltpu.HBM)] * 4,
            out_specs=[pl.BlockSpec(memory_space=pltpu.VMEM)] * 2,
            scratch_shapes=[
                pltpu.VMEM((8, planes + 6) + tile, F32),
                pltpu.VMEM((8,) + tile, F32),
                pltpu.VMEM((3, planes) + tile, F32),
                pltpu.VMEM((3, planes) + tile, F32),
                pltpu.VMEM((1, lanes), jnp.int32),
                pltpu.VMEM((planes,) + tile, F32),
                pltpu.VMEM((8, 10) + tile, F32),
                pltpu.VMEM((8, 3) + tile, F32),
                pltpu.VMEM((8,) + tile, F32),
                pltpu.VMEM((8,) + tile, F32),
                pltpu.VMEM((8,) + tile, F32),
                pltpu.VMEM((10, 10) + tile, F32),
                pltpu.VMEM((5, 5) + tile, F32),
                pltpu.VMEM((5, planes) + tile, F32),
                pltpu.SemaphoreType.REGULAR((5,)),
                pltpu.SemaphoreType.DMA((6,)),
                pltpu.SemaphoreType.DMA((2 * N_SEMS,)),
                pltpu.SemaphoreType.DMA((2 * N_SEMS,)),
            ],
            compiler_params=pltpu.CompilerParams(
                collective_id=0, has_side_effects=True, vmem_limit_bytes=8 * 1024 * 1024
            ),
            cost_estimate=pl.CostEstimate(
                flops=60_000_000, bytes_accessed=500_000, transcendentals=0
            ),
        )(*[pltpu.with_memory_space_constraint(x, pltpu.HBM) for x in operands])
        return pl.pallas_call(
            store,
            out_shape=[jax.ShapeDtypeStruct(conserved.shape, F32)] * 2,
            in_specs=[pl.BlockSpec(memory_space=pltpu.VMEM)] * 2,
            out_specs=[pl.BlockSpec(memory_space=pltpu.HBM)] * 2,
            scratch_shapes=[pltpu.SemaphoreType.DMA((2,))],
            compiler_params=pltpu.CompilerParams(vmem_limit_bytes=1024 * 1024),
        )(*results)

    placed = (P(None, "gz", "gy", "gx"), P(None, "gz", "gy", "gx"), P("gz", "gy", "gx"), P("gx"))
    return jax.shard_map(
        local,
        mesh=mesh,
        in_specs=placed,
        out_specs=(P(None, "gz", "gy", "gx"), P(None, "gz", "gy", "gx")),
        check_vma=False,
    )
```

```python
import functools

import jax
import jax.numpy as jnp
from jax import lax
from jax.experimental import pallas as pl
from jax.experimental.pallas import tpu as pltpu
from jax.sharding import PartitionSpec as P

GAMMA = 1.4
WENO_EPS = 1e-06
STEP_SIZE = 0.08
MESH = pl.DeviceIdType.MESH
F32 = jnp.float32

Z_DOWN, Z_UP, Y_DOWN, Y_UP, MIRROR, X_DOWN, X_UP, Z_LAST, RELAY, N_SEMS = 0, 3, 6, 9, 12, 15, 16, 17, 18, 21


def recip(value):
    return 1.0 / value


def dot3(first, second):
    return first[0] * second[0] + first[1] * second[1] + first[2] * second[2]


def cell_terms(flow, row):
    density, momentum, energy = flow[0], flow[1:4], flow[4]
    inverse = recip(density)
    velocity = [part * inverse for part in momentum]
    pressure = (GAMMA - 1.0) * energy - (0.5 * (GAMMA - 1.0)) * dot3(momentum, velocity)
    contra = dot3(row, velocity)
    flux = [density * contra]
    flux += [momentum[j] * contra + row[j] * pressure for j in range(3)]
    flux += [(energy + pressure) * contra]
    squared = (GAMMA * pressure * inverse) * dot3(row, row)
    speed = jnp.abs(contra) + squared * lax.rsqrt(squared)
    return velocity, pressure, flux, speed


def weno_part(d0, d1, d2, d3):
    x0, x1, x2 = d1 - d0, d2 - d1, d3 - d2
    e1, e2 = 0.75 * d1, 0.75 * d2
    eps = 3.0 * WENO_EPS
    b0 = (x0 * x0 + eps) + e1 * (x0 + d1)
    b1 = (x1 * x1 + eps) + e1 * d2
    b2 = (x2 * x2 + eps) + e2 * (d2 - x2)
    t12, t02, t01 = b1 * b2, b0 * b2, b0 * b1
    s12, s02, s01 = t12 * t12, t02 * t02, t01 * t01
    w2 = 1.5 * s01
    total = (s12 + 6.0 * s02) + (w2 + w2)
    top = s12 * (x0 - x1) + w2 * (x1 - x2)
    return top * recip(total)


def face_flux(d_flow, d_flux, flux_low, alpha, state, row, sweep):
    e, a, b = (sweep + 1) % 3, (sweep + 2) % 3, sweep
    density, velocity, pressure = state
    inverse_density = recip(density)
    sound2 = GAMMA * pressure * inverse_density
    inverse_sound = lax.rsqrt(sound2)
    sound = sound2 * inverse_sound
    inverse_size = lax.rsqrt(dot3(row, row))
    normal = [row[j] * inverse_size for j in range(3)]
    cross_size = lax.rsqrt(row[a] * row[a] + row[b] * row[b])
    l_a, l_b = row[b] * cross_size, -(row[a] * cross_size)
    m_e = normal[a] * l_b - normal[b] * l_a
    m_a = -(normal[e] * l_b)
    m_b = normal[e] * l_a
    kinetic = 0.5 * dot3(velocity, velocity)
    half_factor = (0.5 * (GAMMA - 1.0)) * inverse_sound * inverse_sound
    half_normal = [(0.5 * inverse_sound) * normal[j] for j in range(3)]

    def project(vector):
        rho = vector[0]
        w = [vector[1 + j] - velocity[j] * rho for j in range(3)]
        half_a = half_factor * ((vector[4] - kinetic * rho) - dot3(velocity, w))
        half_n = dot3(half_normal, w)
        return [
            half_a - half_n,
            rho - (half_a + half_a),
            l_a * w[a] + l_b * w[b],
            m_e * w[e] + m_a * w[a] + m_b * w[b],
            half_a + half_n,
        ]

    scaled = [[alpha * d_flow(m, c) for c in range(5)] for m in range(5)]
    ups = [[scaled[m][c] + d_flux(m, c) for c in range(5)] for m in range(4)]
    downs = [[scaled[m][c] - d_flux(m, c) for c in range(5)] for m in range(1, 5)]
    up_chars = [project(vector) for vector in ups]
    down_chars = [project(vector) for vector in downs]
    chars = [
        weno_part(*[up_chars[m][r] for m in range(4)])
        + weno_part(*[down_chars[m][r] for m in (3, 2, 1, 0)])
        for r in range(5)
    ]
    both = chars[0] + chars[4]
    carried = sound * (chars[4] - chars[0])
    mass = both + chars[1]
    enthalpy = sound2 * (1.0 / (GAMMA - 1.0)) + kinetic
    tangent_speed = l_a * velocity[a] + l_b * velocity[b]
    binormal_speed = m_e * velocity[e] + m_a * velocity[a] + m_b * velocity[b]
    right = [None] * 5
    right[0] = mass
    right[1 + e] = velocity[e] * mass + normal[e] * carried + m_e * chars[3]
    right[1 + a] = (velocity[a] * mass + normal[a] * carried) + (l_a * chars[2] + m_a * chars[3])
    right[1 + b] = (velocity[b] * mass + normal[b] * carried) + (l_b * chars[2] + m_b * chars[3])
    right[4] = (enthalpy * both + kinetic * chars[1]) + (
        (tangent_speed * chars[2] + binormal_speed * chars[3]) + dot3(normal, velocity) * carried
    )
    return [
        (flux_low[c] + 0.5 * d_flux(2, c))
        + (1.0 / 6.0) * ((0.5 * (ups[1][c] + downs[2][c]) - scaled[2][c]) + right[c])
        for c in range(5)
    ]


def line_steps(cells, terms, faces, sweep):
    def prepare(k, _):
        flow = [cells[c, k] for c in range(5)]
        row = [cells[5 + j, k] for j in range(3)]
        velocity, pressure, flux, speed = cell_terms(flow, row)
        for c in range(5):
            terms[c, k] = flux[c]
        terms[5, k] = speed
        for j in range(3):
            terms[6 + j, k] = velocity[j]
        terms[9, k] = pressure
        return _

    def one_face(k, _):
        alpha = terms[5, k]
        for m in range(1, 6):
            alpha = jnp.maximum(alpha, terms[5, k + m])
        density = 0.5 * (cells[0, k + 2] + cells[0, k + 3])
        velocity = [0.5 * (terms[6 + j, k + 2] + terms[6 + j, k + 3]) for j in range(3)]
        pressure = 0.5 * (terms[9, k + 2] + terms[9, k + 3])
        row = [0.5 * (cells[5 + j, k + 2] + cells[5 + j, k + 3]) for j in range(3)]
        flux = face_flux(
            lambda m, c: cells[c, k + m + 1] - cells[c, k + m],
            lambda m, c: terms[c, k + m + 1] - terms[c, k + m],
            [terms[c, k + 2] for c in range(5)],
            alpha,
            (density, velocity, pressure),
            row,
            sweep,
        )
        for c in range(5):
            faces[c, k] = flux[c]
        return _

    return prepare, one_face


def lane_sweep(flow, row, sweep):
    lanes = flow[0].shape[-1]

    def ahead(value, shift):
        return pltpu.roll(value, (-shift) % lanes, 1)

    velocity, pressure, flux, speed = cell_terms(flow, row)
    pair = jnp.maximum(speed, ahead(speed, 1))
    alpha = jnp.maximum(jnp.maximum(pair, ahead(pair, -2)), ahead(pair, 2))
    mean = lambda value: 0.5 * (value + ahead(value, 1))
    state = (mean(flow[0]), [mean(part) for part in velocity], mean(pressure))
    row_mean = [mean(part) for part in row]
    d_flow = [ahead(part, 1) - part for part in flow]
    d_flux = [ahead(part, 1) - part for part in flux]
    shifted_flow = [[part if m == 2 else ahead(part, m - 2) for part in d_flow] for m in range(5)]
    shifted_flux = [[part if m == 2 else ahead(part, m - 2) for part in d_flux] for m in range(5)]
    return face_flux(
        lambda m, c: shifted_flow[m][c],
        lambda m, c: shifted_flux[m][c],
        flux,
        alpha,
        state,
        row_mean,
        sweep,
    )


def swap_blocks(values, sublane):
    def exchange(first, second, step):
        high = (sublane // step) % 2 == 1
        return (
            jnp.where(high, pltpu.roll(second, step, 0), first),
            jnp.where(high, second, pltpu.roll(first, 8 - step, 0)),
        )

    v0, v1, v2, v3 = values
    v0, v2 = exchange(v0, v2, 2)
    v1, v3 = exchange(v1, v3, 2)
    v0, v1 = exchange(v0, v1, 1)
    v2, v3 = exchange(v2, v3, 1)
    return [v0, v1, v2, v3]


def kernel(
    shape,
    flow_ref,
    metrics_ref,
    inv_ref,
    wake_ref,
    state_ref,
    rate_ref,
    zv,
    relay,
    ym,
    xm,
    wake,
    inv,
    yv,
    mirror,
    edge,
    edge_low,
    edge_high,
    terms,
    faces,
    z_terms,
    z_faces,
    x_faces,
    ready,
    load_sem,
    send_sem,
    recv_sem,
):
    nx, ny, nz = shape
    planes, rows, lanes = flow_ref.shape[1:]
    ix, iy, iz = lax.axis_index("gx"), lax.axis_index("gy"), lax.axis_index("gz")
    partner = nx - 1 - ix
    has_left, has_right = ix > 0, ix < nx - 1
    at_wall, at_top = iy == 0, iy == ny - 1
    z_low = {"gz": lax.rem(iz + nz - 1, nz)}
    z_high = {"gz": lax.rem(iz + 1, nz)}

    barrier = pltpu.get_barrier_semaphore()

    def greet(target):
        pl.semaphore_signal(barrier, inc=1, device_id=target, device_id_type=MESH)

    is_first, is_second, is_last = iz == 0, iz == 1, iz == nz - 1
    mirror_up = at_wall & (partner > ix)
    mirror_down = at_wall & (partner < ix)
    not_first, not_last = jnp.logical_not(is_first), jnp.logical_not(is_last)
    not_wall, not_top = jnp.logical_not(at_wall), jnp.logical_not(at_top)
    x_low, x_high = {"gx": ix - 1}, {"gx": ix + 1}
    y_low, y_high = {"gy": iy - 1}, {"gy": iy + 1}
    opposite = {"gx": partner}

    def when(condition, action):
        pl.when(condition)(action)

    when(not_last, lambda: greet(z_high))
    when(is_first | is_second, lambda: greet({"gz": nz - 1}))
    when(has_right, lambda: greet(x_high))
    when(not_top, lambda: greet(y_high))
    when(mirror_up, lambda: greet(opposite))
    other_core = lax.rem(iy, 2) == 1
    when(other_core, lambda: greet(y_low))

    as_int = lambda flag: flag.astype(jnp.int32)
    pl.semaphore_wait(
        barrier,
        as_int(not_first)
        + 2 * as_int(is_last)
        + as_int(has_left)
        + as_int(not_wall)
        + as_int(mirror_down)
        + as_int(not_top & jnp.logical_not(other_core)),
    )

    lane = lax.broadcasted_iota(jnp.int32, (rows, lanes), 1)
    sublane = lax.broadcasted_iota(jnp.int32, (rows, lanes), 0)

    def remote(src, dst, index, target):
        return pltpu.make_async_remote_copy(
            src_ref=src,
            dst_ref=dst,
            send_sem=send_sem.at[index],
            recv_sem=recv_sem.at[index],
            device_id=target,
            device_id_type=MESH,
        )

    def up_copy(j):
        return remote(zv.at[:, 2 + planes - j], zv.at[:, 2 - j], Z_UP + j, z_high)

    def down_copy(j):
        return remote(zv.at[:, 3 + j], zv.at[:, 3 + planes + j], Z_DOWN + j, z_low)

    def relay_copy(j):
        return pltpu.make_async_remote_copy(
            src_ref=relay if j == 0 else zv.at[:, j - 1],
            dst_ref=zv.at[:, 3 + planes + j],
            send_sem=send_sem.at[RELAY + j],
            recv_sem=recv_sem.at[Z_DOWN + j],
            device_id={"gz": nz - 1},
            device_id_type=MESH,
        )

    extra = remote(zv.at[:, 3], relay, Z_LAST, z_high)
    ups = [up_copy(j) for j in range(3)]
    downs = [down_copy(j) for j in range(3)]
    relays = [relay_copy(j) for j in range(3)]

    def start(copies):
        def action():
            for copy in copies:
                copy.start()

        return action

    def start_wrap():
        for j in range(3):
            plane = planes - 1 - j
            for part, low, high in ((flow_ref.at[:, plane], 0, 5), (metrics_ref.at[6:9, plane], 5, 8)):
                pltpu.make_async_remote_copy(
                    src_ref=part,
                    dst_ref=zv.at[low:high, 2 - j],
                    send_sem=send_sem.at[Z_UP + j],
                    recv_sem=recv_sem.at[Z_UP + j],
                    device_id=z_high,
                    device_id_type=MESH,
                ).start()

    when(is_last, start_wrap)

    def start_downs():
        for j in range(3):
            for part, low, high in ((flow_ref.at[:, j], 0, 5), (metrics_ref.at[6:9, j], 5, 8)):
                pltpu.make_async_remote_copy(
                    src_ref=part,
                    dst_ref=zv.at[low:high, 3 + planes + j],
                    send_sem=send_sem.at[Z_DOWN + j],
                    recv_sem=recv_sem.at[Z_DOWN + j],
                    device_id=z_low,
                    device_id_type=MESH,
                ).start()

    when(not_first & not_last, start_downs)
    loads = [
        pltpu.make_async_copy(flow_ref, zv.at[0:5, 3 : 3 + planes], load_sem.at[0]),
        pltpu.make_async_copy(metrics_ref.at[6:9], zv.at[5:8, 3 : 3 + planes], load_sem.at[1]),
        pltpu.make_async_copy(metrics_ref.at[0:3], xm, load_sem.at[2]),
        pltpu.make_async_copy(metrics_ref.at[3:6], ym, load_sem.at[3]),
        pltpu.make_async_copy(wake_ref, wake, load_sem.at[4]),
        pltpu.make_async_copy(inv_ref, inv, load_sem.at[5]),
    ]
    for copy in loads:
        copy.start()

    def tell(index, target):
        pl.semaphore_signal(ready.at[index], inc=1, device_id=target, device_id_type=MESH)

    def hear(index):
        pl.semaphore_wait(ready.at[index], 1)

    when(not_first, lambda: tell(0, z_low))
    when(is_last, lambda: tell(1, {"gz": 1}))
    when(has_left, lambda: tell(2, x_low))
    when(not_wall, lambda: tell(3, y_low))
    when(mirror_down, lambda: tell(4, opposite))

    for copy in loads[0:2]:
        copy.wait()
    for copy in loads[2:]:
        copy.wait()

    def source(c, p):
        return zv[c, 3 + p] if c < 5 else xm[c - 5, p]

    for c in range(8):
        packed = source(c, planes - 1)
        for p in range(planes):
            value = source(c, p)
            low = pltpu.roll(value, 16 * p + 3, 1)
            high = pltpu.roll(value, (16 * p + 13) % lanes, 1)
            packed = jnp.where((lane >= 16 * p + 3) & (lane < 16 * p + 8), low, packed)
            packed = jnp.where((lane >= 16 * p + 8) & (lane < 16 * p + 13), high, packed)
        edge[c] = packed

    x_down = remote(edge, edge_high, X_DOWN, x_low)
    x_up = remote(edge, edge_low, X_UP, x_high)
    when(has_left, x_down.start)

    def y_copies(kind):
        copies = []
        for j in range(3):
            if kind == "down":
                index, target, cell = Y_DOWN + j, {"gy": iy - 1}, j
                flow_dst = lambda lo, hi: yv.at[lo:hi, 7 + j, 4:8, :]
            elif kind == "up":
                index, target, cell = Y_UP + j, {"gy": iy + 1}, rows - 3 + j
                flow_dst = lambda lo, hi: yv.at[lo:hi, j, 0:4, :]
            else:
                index, target, cell = MIRROR + j, {"gx": partner}, j
                flow_dst = lambda lo, hi: mirror.at[lo:hi, j, 0:4, :]
            copies.append(
                pltpu.make_async_remote_copy(
                    src_ref=zv.at[0:5, 3 : 3 + planes, cell, :],
                    dst_ref=flow_dst(0, 5),
                    send_sem=send_sem.at[index],
                    recv_sem=recv_sem.at[index],
                    device_id=target,
                    device_id_type=MESH,
                )
            )
            copies.append(
                pltpu.make_async_remote_copy(
                    src_ref=ym.at[:, :, cell, :],
                    dst_ref=flow_dst(5, 8),
                    send_sem=send_sem.at[N_SEMS + index],
                    recv_sem=recv_sem.at[N_SEMS + index],
                    device_id=target,
                    device_id_type=MESH,
                )
            )
        return copies

    y_down, y_up, to_mirror = y_copies("down"), y_copies("up"), y_copies("mirror")

    when(not_wall, start(y_down))
    when(mirror_down, start(to_mirror))

    @pl.when(not_last)
    def _():
        hear(0)
        when(is_first, extra.start)
        start([ups[2], ups[1], ups[0]])()

    @pl.when(mirror_up)
    def _():
        hear(4)
        start(to_mirror)()

    @pl.when(not_top)
    def _():
        hear(3)
        start(y_up)()

    @pl.when(has_right)
    def _():
        hear(2)
        x_up.start()

    def x_plane(p, _):
        flux = lane_sweep([zv[c, 3 + p] for c in range(5)], [xm[j, p] for j in range(3)], 0)
        for c in range(5):
            x_faces[c, p] = flux[c]
        return _

    lax.fori_loop(0, planes, x_plane, 0)

    @pl.when(is_second)
    def _():
        hear(1)
        for arriving, leaving in zip((extra, ups[2], ups[1]), relays):
            arriving.wait_recv()
            leaving.start()

    when(is_last, start(downs))

    lower_half = sublane < 4
    for c in range(8):
        swapped = swap_blocks(
            [zv[c, 3 + p] if c < 5 else ym[c - 5, p] for p in range(planes)], sublane
        )
        for k in range(4):
            yv[c, 3 + k] = swapped[k]
        for k in range(3):
            yv[c, k, 4:8] = swapped[1 + k][0:4]
            yv[c, 7 + k, 0:4] = swapped[k][4:8]

    prepare_y, face_y = line_steps(yv, terms, faces, 1)
    prepare_z, face_z = line_steps(zv, z_terms, z_faces, 2)
    lax.fori_loop(3, 3 + planes, prepare_z, 0)
    lax.fori_loop(3, 7, prepare_y, 0)

    @pl.when(jnp.logical_not(at_top))
    def _():
        for copy in y_down:
            copy.wait_recv()

    @pl.when(at_top)
    def _():
        for c in range(8):
            for k in range(3):
                yv[c, 7 + k, 4:8] = yv[c, 6, 4:8]

    lax.fori_loop(7, 10, prepare_y, 0)
    lax.fori_loop(3, 5, face_y, 0)

    @pl.when(jnp.logical_not(at_wall))
    def _():
        for copy in y_up:
            copy.wait_recv()

    @pl.when(at_wall)
    def _():
        for copy in to_mirror:
            copy.wait_recv()
        is_wake = jnp.broadcast_to(wake[...], (rows, lanes)) >= 0
        backwards = (lanes - 1) - lane
        for c in range(8):
            for k in range(3):
                facing = jnp.take_along_axis(
                    mirror[c, k], backwards, axis=1, mode="promise_in_bounds"
                )
                here = yv[c, 3 + k]
                if 1 <= c <= 3:
                    here = -here
                yv[c, 2 - k, 0:4] = jnp.where(is_wake, facing, here)[0:4]

    lax.fori_loop(0, 3, prepare_y, 0)
    lax.fori_loop(0, 3, face_y, 0)
    y_parts = []
    for c in range(5):
        y_parts.append(
            swap_blocks([faces[c, k] - faces[c, k + 1] for k in range(4)], sublane)
        )
    for c in range(5):
        for p in range(planes):
            rate_ref[c, p] = y_parts[c][p]

    @pl.when(has_left)
    def _():
        x_up.wait_recv()

    @pl.when(jnp.logical_not(has_left))
    def _():
        for c in range(8):
            for k in range(3):
                moved = pltpu.roll(edge[c], 7 + k, 1)
                edge_low[c] = moved if k == 0 else jnp.where(lane % 16 == 10 + k, moved, edge_low[c])

    @pl.when(has_right)
    def _():
        x_down.wait_recv()

    @pl.when(jnp.logical_not(has_right))
    def _():
        for c in range(8):
            for k in range(3):
                moved = pltpu.roll(edge[c], (3 + k - 12) % lanes, 1)
                edge_high[c] = moved if k == 0 else jnp.where(lane % 16 == 3 + k, moved, edge_high[c])

    place = lane % 16
    ends = []
    for c in range(8):
        value = jnp.where(place < 3, pltpu.roll(edge_low[c], lanes - 10, 1), edge[c])
        value = jnp.where(place >= 13, pltpu.roll(edge_high[c], 10, 1), value)
        ends.append(value)
    ends = lane_sweep(ends[0:5], ends[5:8], 0)
    for c in range(5):
        for p in range(planes):
            low = pltpu.roll(ends[c], (-(16 * p + 3)) % lanes, 1)
            high = pltpu.roll(ends[c], (lanes - 3 - (16 * p + 10)) % lanes, 1)
            upper = jnp.where(lane < 2, low, jnp.where(lane >= lanes - 3, high, x_faces[c, p]))
            lower = pltpu.roll(jnp.where(lane == lanes - 1, low, upper), 1, 1)
            rate_ref[c, p] = rate_ref[c, p] + (lower - upper)

    below_last = 2 * iz < nz
    pick = lambda low, high: jnp.where(below_last, low, high)

    def arrival(slot, index):
        return remote(zv.at[:, 3], zv.at[:, slot], index, z_high)

    def finish(k, _):
        volume = inv[k]
        for c in range(5):
            rate = volume * (rate_ref[c, k] + (z_faces[c, k] - z_faces[c, k + 1]))
            rate_ref[c, k] = rate
            state_ref[c, k] = zv[c, 3 + k] + STEP_SIZE * rate
        return _

    def soon(j, carry):
        slot = pick(7 + j, 2 - j)
        arrival(slot, pick(Z_DOWN + j, Z_UP + j)).wait_recv()
        return prepare_z(slot, carry)

    lax.fori_loop(0, 3, soon, 0)
    lax.fori_loop(0, 2, lambda j, carry: face_z(pick(3 + j, j), carry), 0)
    finish(pick(3, 0), 0)

    def late(j, carry):
        slot = pick(2 - j, 7 + j)

        @pl.when(jnp.logical_not(is_second) | (j == 0))
        def _():
            arrival(slot, pick(Z_UP + j, Z_DOWN + j)).wait_recv()

        prepare_z(slot, 0)
        face_z(pick(2 - j, 2 + j), 0)
        finish(pick(2 - j, 1 + j), 0)
        return carry

    for copy in ups:
        copy.wait_send()

    @pl.when(is_first)
    def _():
        extra.wait_send()

    @pl.when(jnp.logical_not(is_first))
    def _():
        for copy in downs:
            copy.wait_send()

    @pl.when(has_left)
    def _():
        x_down.wait_send()

    @pl.when(has_right)
    def _():
        x_up.wait_send()

    @pl.when(at_wall)
    def _():
        for copy in to_mirror:
            copy.wait_send()

    @pl.when(jnp.logical_not(at_wall))
    def _():
        for copy in y_down:
            copy.wait_send()

    @pl.when(jnp.logical_not(at_top))
    def _():
        for copy in y_up:
            copy.wait_send()

    lax.fori_loop(0, 3, late, 0)

    @pl.when(is_second)
    def _():
        for copy in relays:
            copy.wait_send()


def store(state_ref, rate_ref, state_out, rate_out, sem):
    copies = [
        pltpu.make_async_copy(state_ref, state_out, sem.at[0]),
        pltpu.make_async_copy(rate_ref, rate_out, sem.at[1]),
    ]
    for copy in copies:
        copy.start()
    for copy in copies:
        copy.wait()


def solution(mesh):
    nx, ny, nz = mesh.shape["gx"], mesh.shape["gy"], mesh.shape["gz"]

    def local(conserved, metrics, inv_volume, wake_donor):
        planes, rows, lanes = conserved.shape[1:]
        tile = (rows, lanes)
        operands = (conserved, metrics, inv_volume, wake_donor.reshape(1, lanes))
        results = pl.pallas_call(
            functools.partial(kernel, (nx, ny, nz)),
            out_shape=[jax.ShapeDtypeStruct(conserved.shape, F32)] * 2,
            in_specs=[pl.BlockSpec(memory_space=pltpu.HBM)] * 4,
            out_specs=[pl.BlockSpec(memory_space=pltpu.VMEM)] * 2,
            scratch_shapes=[
                pltpu.VMEM((8, planes + 6) + tile, F32),
                pltpu.VMEM((8,) + tile, F32),
                pltpu.VMEM((3, planes) + tile, F32),
                pltpu.VMEM((3, planes) + tile, F32),
                pltpu.VMEM((1, lanes), jnp.int32),
                pltpu.VMEM((planes,) + tile, F32),
                pltpu.VMEM((8, 10) + tile, F32),
                pltpu.VMEM((8, 3) + tile, F32),
                pltpu.VMEM((8,) + tile, F32),
                pltpu.VMEM((8,) + tile, F32),
                pltpu.VMEM((8,) + tile, F32),
                pltpu.VMEM((10, 10) + tile, F32),
                pltpu.VMEM((5, 5) + tile, F32),
                pltpu.VMEM((10, planes + 6) + tile, F32),
                pltpu.VMEM((5, planes + 1) + tile, F32),
                pltpu.VMEM((5, planes) + tile, F32),
                pltpu.SemaphoreType.REGULAR((5,)),
                pltpu.SemaphoreType.DMA((6,)),
                pltpu.SemaphoreType.DMA((2 * N_SEMS,)),
                pltpu.SemaphoreType.DMA((2 * N_SEMS,)),
            ],
            compiler_params=pltpu.CompilerParams(
                collective_id=0, has_side_effects=True, vmem_limit_bytes=8 * 1024 * 1024
            ),
            cost_estimate=pl.CostEstimate(
                flops=60_000_000, bytes_accessed=500_000, transcendentals=0
            ),
        )(*[pltpu.with_memory_space_constraint(x, pltpu.HBM) for x in operands])
        return pl.pallas_call(
            store,
            out_shape=[jax.ShapeDtypeStruct(conserved.shape, F32)] * 2,
            in_specs=[pl.BlockSpec(memory_space=pltpu.VMEM)] * 2,
            out_specs=[pl.BlockSpec(memory_space=pltpu.HBM)] * 2,
            scratch_shapes=[pltpu.SemaphoreType.DMA((2,))],
            compiler_params=pltpu.CompilerParams(vmem_limit_bytes=1024 * 1024),
        )(*results)

    placed = (P(None, "gz", "gy", "gx"), P(None, "gz", "gy", "gx"), P("gz", "gy", "gx"), P("gx"))
    return jax.shard_map(
        local,
        mesh=mesh,
        in_specs=placed,
        out_specs=(P(None, "gz", "gy", "gx"), P(None, "gz", "gy", "gx")),
        check_vma=False,
    )
```

```python
import functools

import jax
import jax.numpy as jnp
from jax import lax
from jax.experimental import pallas as pl
from jax.experimental.pallas import tpu as pltpu
from jax.sharding import PartitionSpec as P

GAMMA = 1.4
WENO_EPS = 1e-06
STEP_SIZE = 0.08
MESH = pl.DeviceIdType.MESH
F32 = jnp.float32

Z_DOWN, Z_UP, Y_DOWN, Y_UP, MIRROR, X_DOWN, X_UP, Z_LAST, RELAY, N_SEMS = 0, 3, 6, 9, 12, 15, 16, 17, 18, 21


def recip(value):
    return 1.0 / value


def dot3(first, second):
    return first[0] * second[0] + first[1] * second[1] + first[2] * second[2]


def cell_terms(flow, row):
    density, momentum, energy = flow[0], flow[1:4], flow[4]
    inverse = recip(density)
    velocity = [part * inverse for part in momentum]
    pressure = (GAMMA - 1.0) * energy - (0.5 * (GAMMA - 1.0)) * dot3(momentum, velocity)
    contra = dot3(row, velocity)
    flux = [density * contra]
    flux += [momentum[j] * contra + row[j] * pressure for j in range(3)]
    flux += [(energy + pressure) * contra]
    squared = (GAMMA * pressure * inverse) * dot3(row, row)
    speed = jnp.abs(contra) + squared * lax.rsqrt(squared)
    return velocity, pressure, flux, speed


def weno_part(d0, d1, d2, d3):
    x0, x1, x2 = d1 - d0, d2 - d1, d3 - d2
    e1, e2 = 0.75 * d1, 0.75 * d2
    eps = 3.0 * WENO_EPS
    b0 = (x0 * x0 + eps) + e1 * (x0 + d1)
    b1 = (x1 * x1 + eps) + e1 * d2
    b2 = (x2 * x2 + eps) + e2 * (d2 - x2)
    t12, t02, t01 = b1 * b2, b0 * b2, b0 * b1
    s12, s02, s01 = t12 * t12, t02 * t02, t01 * t01
    w2 = 1.5 * s01
    total = (s12 + 6.0 * s02) + (w2 + w2)
    top = s12 * (x0 - x1) + w2 * (x1 - x2)
    return top * recip(total)


def face_flux(d_flow, d_flux, flux_low, alpha, state, row, sweep):
    e, a, b = (sweep + 1) % 3, (sweep + 2) % 3, sweep
    density, velocity, pressure = state
    inverse_density = recip(density)
    sound2 = GAMMA * pressure * inverse_density
    inverse_sound = lax.rsqrt(sound2)
    sound = sound2 * inverse_sound
    inverse_size = lax.rsqrt(dot3(row, row))
    normal = [row[j] * inverse_size for j in range(3)]
    cross_size = lax.rsqrt(row[a] * row[a] + row[b] * row[b])
    l_a, l_b = row[b] * cross_size, -(row[a] * cross_size)
    m_e = normal[a] * l_b - normal[b] * l_a
    m_a = -(normal[e] * l_b)
    m_b = normal[e] * l_a
    kinetic = 0.5 * dot3(velocity, velocity)
    half_factor = (0.5 * (GAMMA - 1.0)) * inverse_sound * inverse_sound
    half_normal = [(0.5 * inverse_sound) * normal[j] for j in range(3)]

    def project(vector):
        rho = vector[0]
        w = [vector[1 + j] - velocity[j] * rho for j in range(3)]
        half_a = half_factor * ((vector[4] - kinetic * rho) - dot3(velocity, w))
        half_n = dot3(half_normal, w)
        return [
            half_a - half_n,
            rho - (half_a + half_a),
            l_a * w[a] + l_b * w[b],
            m_e * w[e] + m_a * w[a] + m_b * w[b],
            half_a + half_n,
        ]

    scaled = [[alpha * d_flow(m, c) for c in range(5)] for m in range(5)]
    ups = [[scaled[m][c] + d_flux(m, c) for c in range(5)] for m in range(4)]
    downs = [[scaled[m][c] - d_flux(m, c) for c in range(5)] for m in range(1, 5)]
    up_chars = [project(vector) for vector in ups]
    down_chars = [project(vector) for vector in downs]
    chars = [
        weno_part(*[up_chars[m][r] for m in range(4)])
        + weno_part(*[down_chars[m][r] for m in (3, 2, 1, 0)])
        for r in range(5)
    ]
    both = chars[0] + chars[4]
    carried = sound * (chars[4] - chars[0])
    mass = both + chars[1]
    enthalpy = sound2 * (1.0 / (GAMMA - 1.0)) + kinetic
    tangent_speed = l_a * velocity[a] + l_b * velocity[b]
    binormal_speed = m_e * velocity[e] + m_a * velocity[a] + m_b * velocity[b]
    right = [None] * 5
    right[0] = mass
    right[1 + e] = velocity[e] * mass + normal[e] * carried + m_e * chars[3]
    right[1 + a] = (velocity[a] * mass + normal[a] * carried) + (l_a * chars[2] + m_a * chars[3])
    right[1 + b] = (velocity[b] * mass + normal[b] * carried) + (l_b * chars[2] + m_b * chars[3])
    right[4] = (enthalpy * both + kinetic * chars[1]) + (
        (tangent_speed * chars[2] + binormal_speed * chars[3]) + dot3(normal, velocity) * carried
    )
    return [
        (flux_low[c] + 0.5 * d_flux(2, c))
        + (1.0 / 6.0) * ((0.5 * (ups[1][c] + downs[2][c]) - scaled[2][c]) + right[c])
        for c in range(5)
    ]


def line_steps(cells, terms, faces, sweep):
    def prepare(k, _):
        flow = [cells[c, k] for c in range(5)]
        row = [cells[5 + j, k] for j in range(3)]
        velocity, pressure, flux, speed = cell_terms(flow, row)
        for c in range(5):
            terms[c, k] = flux[c]
        terms[5, k] = speed
        for j in range(3):
            terms[6 + j, k] = velocity[j]
        terms[9, k] = pressure
        return _

    def one_face(k, _):
        alpha = terms[5, k]
        for m in range(1, 6):
            alpha = jnp.maximum(alpha, terms[5, k + m])
        density = 0.5 * (cells[0, k + 2] + cells[0, k + 3])
        velocity = [0.5 * (terms[6 + j, k + 2] + terms[6 + j, k + 3]) for j in range(3)]
        pressure = 0.5 * (terms[9, k + 2] + terms[9, k + 3])
        row = [0.5 * (cells[5 + j, k + 2] + cells[5 + j, k + 3]) for j in range(3)]
        flux = face_flux(
            lambda m, c: cells[c, k + m + 1] - cells[c, k + m],
            lambda m, c: terms[c, k + m + 1] - terms[c, k + m],
            [terms[c, k + 2] for c in range(5)],
            alpha,
            (density, velocity, pressure),
            row,
            sweep,
        )
        for c in range(5):
            faces[c, k] = flux[c]
        return _

    return prepare, one_face


def lane_sweep(flow, row, sweep):
    lanes = flow[0].shape[-1]

    def ahead(value, shift):
        return pltpu.roll(value, (-shift) % lanes, 1)

    velocity, pressure, flux, speed = cell_terms(flow, row)
    pair = jnp.maximum(speed, ahead(speed, 1))
    alpha = jnp.maximum(jnp.maximum(pair, ahead(pair, -2)), ahead(pair, 2))
    mean = lambda value: 0.5 * (value + ahead(value, 1))
    state = (mean(flow[0]), [mean(part) for part in velocity], mean(pressure))
    row_mean = [mean(part) for part in row]
    d_flow = [ahead(part, 1) - part for part in flow]
    d_flux = [ahead(part, 1) - part for part in flux]
    shifted_flow = [[part if m == 2 else ahead(part, m - 2) for part in d_flow] for m in range(5)]
    shifted_flux = [[part if m == 2 else ahead(part, m - 2) for part in d_flux] for m in range(5)]
    return face_flux(
        lambda m, c: shifted_flow[m][c],
        lambda m, c: shifted_flux[m][c],
        flux,
        alpha,
        state,
        row_mean,
        sweep,
    )


def swap_blocks(values, sublane):
    def exchange(first, second, step):
        high = (sublane // step) % 2 == 1
        return (
            jnp.where(high, pltpu.roll(second, step, 0), first),
            jnp.where(high, second, pltpu.roll(first, 8 - step, 0)),
        )

    v0, v1, v2, v3 = values
    v0, v2 = exchange(v0, v2, 2)
    v1, v3 = exchange(v1, v3, 2)
    v0, v1 = exchange(v0, v1, 1)
    v2, v3 = exchange(v2, v3, 1)
    return [v0, v1, v2, v3]


def kernel(
    shape,
    flow_ref,
    metrics_ref,
    inv_ref,
    wake_ref,
    state_ref,
    rate_ref,
    zv,
    relay,
    ym,
    xm,
    wake,
    inv,
    yv,
    mirror,
    edge,
    edge_low,
    edge_high,
    terms,
    faces,
    z_terms,
    z_faces,
    x_faces,
    ready,
    load_sem,
    send_sem,
    recv_sem,
):
    nx, ny, nz = shape
    planes, rows, lanes = flow_ref.shape[1:]
    ix, iy, iz = lax.axis_index("gx"), lax.axis_index("gy"), lax.axis_index("gz")
    partner = nx - 1 - ix
    has_left, has_right = ix > 0, ix < nx - 1
    at_wall, at_top = iy == 0, iy == ny - 1
    z_low = {"gz": lax.rem(iz + nz - 1, nz)}
    z_high = {"gz": lax.rem(iz + 1, nz)}

    barrier = pltpu.get_barrier_semaphore()

    def greet(target):
        pl.semaphore_signal(barrier, inc=1, device_id=target, device_id_type=MESH)

    is_first, is_second, is_last = iz == 0, iz == 1, iz == nz - 1
    mirror_up = at_wall & (partner > ix)
    mirror_down = at_wall & (partner < ix)
    not_first, not_last = jnp.logical_not(is_first), jnp.logical_not(is_last)
    not_wall, not_top = jnp.logical_not(at_wall), jnp.logical_not(at_top)
    x_low, x_high = {"gx": ix - 1}, {"gx": ix + 1}
    y_low, y_high = {"gy": iy - 1}, {"gy": iy + 1}
    opposite = {"gx": partner}

    def when(condition, action):
        pl.when(condition)(action)

    when(not_last, lambda: greet(z_high))
    when(is_first | is_second, lambda: greet({"gz": nz - 1}))
    when(has_right, lambda: greet(x_high))
    when(not_top, lambda: greet(y_high))
    when(mirror_up, lambda: greet(opposite))
    other_core = lax.rem(iy, 2) == 1
    when(other_core, lambda: greet(y_low))

    as_int = lambda flag: flag.astype(jnp.int32)
    pl.semaphore_wait(
        barrier,
        as_int(not_first)
        + 2 * as_int(is_last)
        + as_int(has_left)
        + as_int(not_wall)
        + as_int(mirror_down)
        + as_int(not_top & jnp.logical_not(other_core)),
    )

    lane = lax.broadcasted_iota(jnp.int32, (rows, lanes), 1)
    sublane = lax.broadcasted_iota(jnp.int32, (rows, lanes), 0)

    def remote(src, dst, index, target):
        return pltpu.make_async_remote_copy(
            src_ref=src,
            dst_ref=dst,
            send_sem=send_sem.at[index],
            recv_sem=recv_sem.at[index],
            device_id=target,
            device_id_type=MESH,
        )

    def up_copy(j):
        return remote(zv.at[:, 2 + planes - j], zv.at[:, 2 - j], Z_UP + j, z_high)

    def down_copy(j):
        return remote(zv.at[:, 3 + j], zv.at[:, 3 + planes + j], Z_DOWN + j, z_low)

    def relay_copy(j):
        return pltpu.make_async_remote_copy(
            src_ref=relay if j == 0 else zv.at[:, j - 1],
            dst_ref=zv.at[:, 3 + planes + j],
            send_sem=send_sem.at[RELAY + j],
            recv_sem=recv_sem.at[Z_DOWN + j],
            device_id={"gz": nz - 1},
            device_id_type=MESH,
        )

    extra = remote(zv.at[:, 3], relay, Z_LAST, z_high)
    ups = [up_copy(j) for j in range(3)]
    downs = [down_copy(j) for j in range(3)]
    relays = [relay_copy(j) for j in range(3)]

    def start(copies):
        def action():
            for copy in copies:
                copy.start()

        return action

    def start_wrap(count):
        for j in count:
            plane = planes - 1 - j
            for part, low, high in ((flow_ref.at[:, plane], 0, 5), (metrics_ref.at[6:9, plane], 5, 8)):
                pltpu.make_async_remote_copy(
                    src_ref=part,
                    dst_ref=zv.at[low:high, 2 - j],
                    send_sem=send_sem.at[Z_UP + j],
                    recv_sem=recv_sem.at[Z_UP + j],
                    device_id=z_high,
                    device_id_type=MESH,
                ).start()

    when(is_last, lambda: start_wrap((0,)))
    when(is_last & jnp.logical_not(other_core), lambda: start_wrap((1, 2)))

    def start_downs():
        for j in range(3):
            for part, low, high in ((flow_ref.at[:, j], 0, 5), (metrics_ref.at[6:9, j], 5, 8)):
                pltpu.make_async_remote_copy(
                    src_ref=part,
                    dst_ref=zv.at[low:high, 3 + planes + j],
                    send_sem=send_sem.at[Z_DOWN + j],
                    recv_sem=recv_sem.at[Z_DOWN + j],
                    device_id=z_low,
                    device_id_type=MESH,
                ).start()

    def y_copies(kind, early):
        flow = flow_ref if early else zv.at[0:5, 3 : 3 + planes]
        row = metrics_ref.at[3:6] if early else ym
        copies = []
        for j in range(3):
            if kind == "down":
                index, target, cell = Y_DOWN + j, {"gy": iy - 1}, j
                flow_dst = lambda lo, hi: yv.at[lo:hi, 7 + j, 4:8, :]
            elif kind == "up":
                index, target, cell = Y_UP + j, {"gy": iy + 1}, rows - 3 + j
                flow_dst = lambda lo, hi: yv.at[lo:hi, j, 0:4, :]
            else:
                index, target, cell = MIRROR + j, {"gx": partner}, j
                flow_dst = lambda lo, hi: mirror.at[lo:hi, j, 0:4, :]
            copies.append(
                pltpu.make_async_remote_copy(
                    src_ref=flow.at[:, :, cell, :],
                    dst_ref=flow_dst(0, 5),
                    send_sem=send_sem.at[index],
                    recv_sem=recv_sem.at[index],
                    device_id=target,
                    device_id_type=MESH,
                )
            )
            copies.append(
                pltpu.make_async_remote_copy(
                    src_ref=row.at[:, :, cell, :],
                    dst_ref=flow_dst(5, 8),
                    send_sem=send_sem.at[N_SEMS + index],
                    recv_sem=recv_sem.at[N_SEMS + index],
                    device_id=target,
                    device_id_type=MESH,
                )
            )
        return copies

    y_down, y_up = y_copies("down", True), y_copies("up", False)
    to_mirror = y_copies("mirror", False)

    when(not_first & not_last, start_downs)
    when(mirror_down, start(y_copies("mirror", True)))
    when(not_wall, start(y_down))
    loads = [
        pltpu.make_async_copy(flow_ref, zv.at[0:5, 3 : 3 + planes], load_sem.at[0]),
        pltpu.make_async_copy(metrics_ref.at[6:9], zv.at[5:8, 3 : 3 + planes], load_sem.at[1]),
        pltpu.make_async_copy(metrics_ref.at[0:3], xm, load_sem.at[2]),
        pltpu.make_async_copy(metrics_ref.at[3:6], ym, load_sem.at[3]),
        pltpu.make_async_copy(wake_ref, wake, load_sem.at[4]),
        pltpu.make_async_copy(inv_ref, inv, load_sem.at[5]),
    ]
    for copy in loads:
        copy.start()

    def tell(index, target):
        pl.semaphore_signal(ready.at[index], inc=1, device_id=target, device_id_type=MESH)

    def hear(index):
        pl.semaphore_wait(ready.at[index], 1)

    when(not_first, lambda: tell(0, z_low))
    when(is_last, lambda: tell(1, {"gz": 1}))
    when(has_left, lambda: tell(2, x_low))
    when(not_wall, lambda: tell(3, y_low))
    when(mirror_down, lambda: tell(4, opposite))

    for copy in loads[0:2]:
        copy.wait()
    for copy in loads[2:]:
        copy.wait()

    def source(c, p):
        return zv[c, 3 + p] if c < 5 else xm[c - 5, p]

    for c in range(8):
        packed = source(c, planes - 1)
        for p in range(planes):
            value = source(c, p)
            low = pltpu.roll(value, 16 * p + 3, 1)
            high = pltpu.roll(value, (16 * p + 13) % lanes, 1)
            packed = jnp.where((lane >= 16 * p + 3) & (lane < 16 * p + 8), low, packed)
            packed = jnp.where((lane >= 16 * p + 8) & (lane < 16 * p + 13), high, packed)
        edge[c] = packed

    x_down = remote(edge, edge_high, X_DOWN, x_low)
    x_up = remote(edge, edge_low, X_UP, x_high)
    when(has_left, x_down.start)

    @pl.when(not_last)
    def _():
        hear(0)
        when(is_first, extra.start)
        start([ups[2], ups[1], ups[0]])()

    @pl.when(mirror_up)
    def _():
        hear(4)
        start(to_mirror)()

    @pl.when(not_top)
    def _():
        hear(3)
        start(y_up)()

    @pl.when(has_right)
    def _():
        hear(2)
        x_up.start()

    def x_plane(p, _):
        when(is_last & other_core & (p == 1), start(ups[1:]))
        flux = lane_sweep([zv[c, 3 + p] for c in range(5)], [xm[j, p] for j in range(3)], 0)
        for c in range(5):
            x_faces[c, p] = flux[c]
        return _

    lax.fori_loop(0, planes, x_plane, 0)

    @pl.when(is_second)
    def _():
        hear(1)
        for arriving, leaving in zip((extra, ups[2], ups[1]), relays):
            arriving.wait_recv()
            leaving.start()

    when(is_last, start(downs))

    lower_half = sublane < 4
    for c in range(8):
        swapped = swap_blocks(
            [zv[c, 3 + p] if c < 5 else ym[c - 5, p] for p in range(planes)], sublane
        )
        for k in range(4):
            yv[c, 3 + k] = swapped[k]
        for k in range(3):
            yv[c, k, 4:8] = swapped[1 + k][0:4]
            yv[c, 7 + k, 0:4] = swapped[k][4:8]

    prepare_y, face_y = line_steps(yv, terms, faces, 1)
    prepare_z, face_z = line_steps(zv, z_terms, z_faces, 2)
    lax.fori_loop(3, 3 + planes, prepare_z, 0)
    lax.fori_loop(3, 7, prepare_y, 0)

    @pl.when(jnp.logical_not(at_top))
    def _():
        for copy in y_down:
            copy.wait_recv()

    @pl.when(at_top)
    def _():
        for c in range(8):
            for k in range(3):
                yv[c, 7 + k, 4:8] = yv[c, 6, 4:8]

    lax.fori_loop(7, 10, prepare_y, 0)
    lax.fori_loop(3, 5, face_y, 0)

    @pl.when(jnp.logical_not(at_wall))
    def _():
        for copy in y_up:
            copy.wait_recv()

    @pl.when(at_wall)
    def _():
        for copy in to_mirror:
            copy.wait_recv()
        is_wake = jnp.broadcast_to(wake[...], (rows, lanes)) >= 0
        backwards = (lanes - 1) - lane
        for c in range(8):
            for k in range(3):
                facing = jnp.take_along_axis(
                    mirror[c, k], backwards, axis=1, mode="promise_in_bounds"
                )
                here = yv[c, 3 + k]
                if 1 <= c <= 3:
                    here = -here
                yv[c, 2 - k, 0:4] = jnp.where(is_wake, facing, here)[0:4]

    lax.fori_loop(0, 3, prepare_y, 0)
    lax.fori_loop(0, 3, face_y, 0)
    y_parts = []
    for c in range(5):
        y_parts.append(
            swap_blocks([faces[c, k] - faces[c, k + 1] for k in range(4)], sublane)
        )
    for c in range(5):
        for p in range(planes):
            rate_ref[c, p] = y_parts[c][p]

    @pl.when(has_left)
    def _():
        x_up.wait_recv()

    @pl.when(jnp.logical_not(has_left))
    def _():
        for c in range(8):
            for k in range(3):
                moved = pltpu.roll(edge[c], 7 + k, 1)
                edge_low[c] = moved if k == 0 else jnp.where(lane % 16 == 10 + k, moved, edge_low[c])

    @pl.when(has_right)
    def _():
        x_down.wait_recv()

    @pl.when(jnp.logical_not(has_right))
    def _():
        for c in range(8):
            for k in range(3):
                moved = pltpu.roll(edge[c], (3 + k - 12) % lanes, 1)
                edge_high[c] = moved if k == 0 else jnp.where(lane % 16 == 3 + k, moved, edge_high[c])

    place = lane % 16
    ends = []
    for c in range(8):
        value = jnp.where(place < 3, pltpu.roll(edge_low[c], lanes - 10, 1), edge[c])
        value = jnp.where(place >= 13, pltpu.roll(edge_high[c], 10, 1), value)
        ends.append(value)
    ends = lane_sweep(ends[0:5], ends[5:8], 0)
    for c in range(5):
        for p in range(planes):
            low = pltpu.roll(ends[c], (-(16 * p + 3)) % lanes, 1)
            high = pltpu.roll(ends[c], (lanes - 3 - (16 * p + 10)) % lanes, 1)
            upper = jnp.where(lane < 2, low, jnp.where(lane >= lanes - 3, high, x_faces[c, p]))
            lower = pltpu.roll(jnp.where(lane == lanes - 1, low, upper), 1, 1)
            rate_ref[c, p] = rate_ref[c, p] + (lower - upper)

    below_last = 2 * iz < nz
    pick = lambda low, high: jnp.where(below_last, low, high)

    def arrival(slot, index):
        return remote(zv.at[:, 3], zv.at[:, slot], index, z_high)

    def finish(k, _):
        volume = inv[k]
        for c in range(5):
            rate = volume * (rate_ref[c, k] + (z_faces[c, k] - z_faces[c, k + 1]))
            rate_ref[c, k] = rate
            state_ref[c, k] = zv[c, 3 + k] + STEP_SIZE * rate
        return _

    def soon(j, carry):
        slot = pick(7 + j, 2 - j)
        arrival(slot, pick(Z_DOWN + j, Z_UP + j)).wait_recv()
        return prepare_z(slot, carry)

    lax.fori_loop(0, 3, soon, 0)
    lax.fori_loop(0, 2, lambda j, carry: face_z(pick(3 + j, j), carry), 0)
    finish(pick(3, 0), 0)

    def late(j, carry):
        slot = pick(2 - j, 7 + j)

        @pl.when(jnp.logical_not(is_second) | (j == 0))
        def _():
            arrival(slot, pick(Z_UP + j, Z_DOWN + j)).wait_recv()

        prepare_z(slot, 0)
        face_z(pick(2 - j, 2 + j), 0)
        finish(pick(2 - j, 1 + j), 0)
        return carry

    for copy in ups:
        copy.wait_send()

    @pl.when(is_first)
    def _():
        extra.wait_send()

    @pl.when(jnp.logical_not(is_first))
    def _():
        for copy in downs:
            copy.wait_send()

    @pl.when(has_left)
    def _():
        x_down.wait_send()

    @pl.when(has_right)
    def _():
        x_up.wait_send()

    @pl.when(at_wall)
    def _():
        for copy in to_mirror:
            copy.wait_send()

    @pl.when(jnp.logical_not(at_wall))
    def _():
        for copy in y_down:
            copy.wait_send()

    @pl.when(jnp.logical_not(at_top))
    def _():
        for copy in y_up:
            copy.wait_send()

    lax.fori_loop(0, 3, late, 0)

    @pl.when(is_second)
    def _():
        for copy in relays:
            copy.wait_send()


def store(state_ref, rate_ref, state_out, rate_out, sem):
    copies = [
        pltpu.make_async_copy(state_ref, state_out, sem.at[0]),
        pltpu.make_async_copy(rate_ref, rate_out, sem.at[1]),
    ]
    for copy in copies:
        copy.start()
    for copy in copies:
        copy.wait()


def solution(mesh):
    nx, ny, nz = mesh.shape["gx"], mesh.shape["gy"], mesh.shape["gz"]

    def local(conserved, metrics, inv_volume, wake_donor):
        planes, rows, lanes = conserved.shape[1:]
        tile = (rows, lanes)
        operands = (conserved, metrics, inv_volume, wake_donor.reshape(1, lanes))
        results = pl.pallas_call(
            functools.partial(kernel, (nx, ny, nz)),
            out_shape=[jax.ShapeDtypeStruct(conserved.shape, F32)] * 2,
            in_specs=[pl.BlockSpec(memory_space=pltpu.HBM)] * 4,
            out_specs=[pl.BlockSpec(memory_space=pltpu.VMEM)] * 2,
            scratch_shapes=[
                pltpu.VMEM((8, planes + 6) + tile, F32),
                pltpu.VMEM((8,) + tile, F32),
                pltpu.VMEM((3, planes) + tile, F32),
                pltpu.VMEM((3, planes) + tile, F32),
                pltpu.VMEM((1, lanes), jnp.int32),
                pltpu.VMEM((planes,) + tile, F32),
                pltpu.VMEM((8, 10) + tile, F32),
                pltpu.VMEM((8, 3) + tile, F32),
                pltpu.VMEM((8,) + tile, F32),
                pltpu.VMEM((8,) + tile, F32),
                pltpu.VMEM((8,) + tile, F32),
                pltpu.VMEM((10, 10) + tile, F32),
                pltpu.VMEM((5, 5) + tile, F32),
                pltpu.VMEM((10, planes + 6) + tile, F32),
                pltpu.VMEM((5, planes + 1) + tile, F32),
                pltpu.VMEM((5, planes) + tile, F32),
                pltpu.SemaphoreType.REGULAR((5,)),
                pltpu.SemaphoreType.DMA((6,)),
                pltpu.SemaphoreType.DMA((2 * N_SEMS,)),
                pltpu.SemaphoreType.DMA((2 * N_SEMS,)),
            ],
            compiler_params=pltpu.CompilerParams(
                collective_id=0, has_side_effects=True, vmem_limit_bytes=8 * 1024 * 1024
            ),
            cost_estimate=pl.CostEstimate(
                flops=60_000_000, bytes_accessed=500_000, transcendentals=0
            ),
        )(*[pltpu.with_memory_space_constraint(x, pltpu.HBM) for x in operands])
        return pl.pallas_call(
            store,
            out_shape=[jax.ShapeDtypeStruct(conserved.shape, F32)] * 2,
            in_specs=[pl.BlockSpec(memory_space=pltpu.VMEM)] * 2,
            out_specs=[pl.BlockSpec(memory_space=pltpu.HBM)] * 2,
            scratch_shapes=[pltpu.SemaphoreType.DMA((2,))],
            compiler_params=pltpu.CompilerParams(vmem_limit_bytes=1024 * 1024),
        )(*results)

    placed = (P(None, "gz", "gy", "gx"), P(None, "gz", "gy", "gx"), P("gz", "gy", "gx"), P("gx"))
    return jax.shard_map(
        local,
        mesh=mesh,
        in_specs=placed,
        out_specs=(P(None, "gz", "gy", "gx"), P(None, "gz", "gy", "gx")),
        check_vma=False,
    )
```

```python
import functools

import jax
import jax.numpy as jnp
from jax import lax
from jax.experimental import pallas as pl
from jax.experimental.pallas import tpu as pltpu
from jax.sharding import PartitionSpec as P

GAMMA = 1.4
WENO_EPS = 1e-06
STEP_SIZE = 0.08
MESH = pl.DeviceIdType.MESH
F32 = jnp.float32

Z_DOWN, Z_UP, Y_DOWN, Y_UP, MIRROR, X_DOWN, X_UP, Z_LAST, RELAY, N_SEMS = 0, 3, 6, 9, 12, 15, 16, 17, 18, 21


def recip(value):
    return 1.0 / value


def dot3(first, second):
    return first[0] * second[0] + first[1] * second[1] + first[2] * second[2]


def cell_terms(flow, row):
    density, momentum, energy = flow[0], flow[1:4], flow[4]
    inverse = recip(density)
    velocity = [part * inverse for part in momentum]
    pressure = (GAMMA - 1.0) * energy - (0.5 * (GAMMA - 1.0)) * dot3(momentum, velocity)
    contra = dot3(row, velocity)
    flux = [density * contra]
    flux += [momentum[j] * contra + row[j] * pressure for j in range(3)]
    flux += [(energy + pressure) * contra]
    squared = (GAMMA * pressure * inverse) * dot3(row, row)
    speed = jnp.abs(contra) + squared * lax.rsqrt(squared)
    return velocity, pressure, flux, speed


def weno_part(d0, d1, d2, d3):
    x0, x1, x2 = d1 - d0, d2 - d1, d3 - d2
    e1, e2 = 0.75 * d1, 0.75 * d2
    eps = 3.0 * WENO_EPS
    b0 = (x0 * x0 + eps) + e1 * (x0 + d1)
    b1 = (x1 * x1 + eps) + e1 * d2
    b2 = (x2 * x2 + eps) + e2 * (d2 - x2)
    t12, t02, t01 = b1 * b2, b0 * b2, b0 * b1
    s12, s02, s01 = t12 * t12, t02 * t02, t01 * t01
    w2 = 1.5 * s01
    total = (s12 + 6.0 * s02) + (w2 + w2)
    top = s12 * (x0 - x1) + w2 * (x1 - x2)
    return top * recip(total)


def face_flux(d_flow, d_flux, flux_low, alpha, state, row, sweep):
    e, a, b = (sweep + 1) % 3, (sweep + 2) % 3, sweep
    density, velocity, pressure = state
    inverse_density = recip(density)
    sound2 = GAMMA * pressure * inverse_density
    inverse_sound = lax.rsqrt(sound2)
    sound = sound2 * inverse_sound
    inverse_size = lax.rsqrt(dot3(row, row))
    normal = [row[j] * inverse_size for j in range(3)]
    cross_size = lax.rsqrt(row[a] * row[a] + row[b] * row[b])
    l_a, l_b = row[b] * cross_size, -(row[a] * cross_size)
    m_e = normal[a] * l_b - normal[b] * l_a
    m_a = -(normal[e] * l_b)
    m_b = normal[e] * l_a
    kinetic = 0.5 * dot3(velocity, velocity)
    half_factor = (0.5 * (GAMMA - 1.0)) * inverse_sound * inverse_sound
    half_normal = [(0.5 * inverse_sound) * normal[j] for j in range(3)]

    def project(vector):
        rho = vector[0]
        w = [vector[1 + j] - velocity[j] * rho for j in range(3)]
        half_a = half_factor * ((vector[4] - kinetic * rho) - dot3(velocity, w))
        half_n = dot3(half_normal, w)
        return [
            half_a - half_n,
            rho - (half_a + half_a),
            l_a * w[a] + l_b * w[b],
            m_e * w[e] + m_a * w[a] + m_b * w[b],
            half_a + half_n,
        ]

    scaled = [[alpha * d_flow(m, c) for c in range(5)] for m in range(5)]
    ups = [[scaled[m][c] + d_flux(m, c) for c in range(5)] for m in range(4)]
    downs = [[scaled[m][c] - d_flux(m, c) for c in range(5)] for m in range(1, 5)]
    up_chars = [project(vector) for vector in ups]
    down_chars = [project(vector) for vector in downs]
    chars = [
        weno_part(*[up_chars[m][r] for m in range(4)])
        + weno_part(*[down_chars[m][r] for m in (3, 2, 1, 0)])
        for r in range(5)
    ]
    both = chars[0] + chars[4]
    carried = sound * (chars[4] - chars[0])
    mass = both + chars[1]
    enthalpy = sound2 * (1.0 / (GAMMA - 1.0)) + kinetic
    tangent_speed = l_a * velocity[a] + l_b * velocity[b]
    binormal_speed = m_e * velocity[e] + m_a * velocity[a] + m_b * velocity[b]
    right = [None] * 5
    right[0] = mass
    right[1 + e] = velocity[e] * mass + normal[e] * carried + m_e * chars[3]
    right[1 + a] = (velocity[a] * mass + normal[a] * carried) + (l_a * chars[2] + m_a * chars[3])
    right[1 + b] = (velocity[b] * mass + normal[b] * carried) + (l_b * chars[2] + m_b * chars[3])
    right[4] = (enthalpy * both + kinetic * chars[1]) + (
        (tangent_speed * chars[2] + binormal_speed * chars[3]) + dot3(normal, velocity) * carried
    )
    return [
        (flux_low[c] + 0.5 * d_flux(2, c))
        + (1.0 / 6.0) * ((0.5 * (ups[1][c] + downs[2][c]) - scaled[2][c]) + right[c])
        for c in range(5)
    ]


def line_steps(cells, terms, faces, sweep):
    def prepare(k, _):
        flow = [cells[c, k] for c in range(5)]
        row = [cells[5 + j, k] for j in range(3)]
        velocity, pressure, flux, speed = cell_terms(flow, row)
        for c in range(5):
            terms[c, k] = flux[c]
        terms[5, k] = speed
        for j in range(3):
            terms[6 + j, k] = velocity[j]
        terms[9, k] = pressure
        return _

    def one_face(k, _):
        alpha = terms[5, k]
        for m in range(1, 6):
            alpha = jnp.maximum(alpha, terms[5, k + m])
        density = 0.5 * (cells[0, k + 2] + cells[0, k + 3])
        velocity = [0.5 * (terms[6 + j, k + 2] + terms[6 + j, k + 3]) for j in range(3)]
        pressure = 0.5 * (terms[9, k + 2] + terms[9, k + 3])
        row = [0.5 * (cells[5 + j, k + 2] + cells[5 + j, k + 3]) for j in range(3)]
        flux = face_flux(
            lambda m, c: cells[c, k + m + 1] - cells[c, k + m],
            lambda m, c: terms[c, k + m + 1] - terms[c, k + m],
            [terms[c, k + 2] for c in range(5)],
            alpha,
            (density, velocity, pressure),
            row,
            sweep,
        )
        for c in range(5):
            faces[c, k] = flux[c]
        return _

    return prepare, one_face


def lane_sweep(flow, row, sweep):
    lanes = flow[0].shape[-1]

    def ahead(value, shift):
        return pltpu.roll(value, (-shift) % lanes, 1)

    velocity, pressure, flux, speed = cell_terms(flow, row)
    pair = jnp.maximum(speed, ahead(speed, 1))
    alpha = jnp.maximum(jnp.maximum(pair, ahead(pair, -2)), ahead(pair, 2))
    mean = lambda value: 0.5 * (value + ahead(value, 1))
    state = (mean(flow[0]), [mean(part) for part in velocity], mean(pressure))
    row_mean = [mean(part) for part in row]
    d_flow = [ahead(part, 1) - part for part in flow]
    d_flux = [ahead(part, 1) - part for part in flux]
    shifted_flow = [[part if m == 2 else ahead(part, m - 2) for part in d_flow] for m in range(5)]
    shifted_flux = [[part if m == 2 else ahead(part, m - 2) for part in d_flux] for m in range(5)]
    return face_flux(
        lambda m, c: shifted_flow[m][c],
        lambda m, c: shifted_flux[m][c],
        flux,
        alpha,
        state,
        row_mean,
        sweep,
    )


def swap_blocks(values, sublane):
    def exchange(first, second, step):
        high = (sublane // step) % 2 == 1
        return (
            jnp.where(high, pltpu.roll(second, step, 0), first),
            jnp.where(high, second, pltpu.roll(first, 8 - step, 0)),
        )

    v0, v1, v2, v3 = values
    v0, v2 = exchange(v0, v2, 2)
    v1, v3 = exchange(v1, v3, 2)
    v0, v1 = exchange(v0, v1, 1)
    v2, v3 = exchange(v2, v3, 1)
    return [v0, v1, v2, v3]


def kernel(
    shape,
    flow_ref,
    metrics_ref,
    inv_ref,
    wake_ref,
    state_ref,
    rate_ref,
    zv,
    relay,
    ym,
    xm,
    wake,
    inv,
    yv,
    mirror,
    edge,
    edge_low,
    edge_high,
    terms,
    faces,
    z_terms,
    z_faces,
    x_faces,
    ready,
    load_sem,
    send_sem,
    recv_sem,
):
    nx, ny, nz = shape
    planes, rows, lanes = flow_ref.shape[1:]
    ix, iy, iz = lax.axis_index("gx"), lax.axis_index("gy"), lax.axis_index("gz")
    partner = nx - 1 - ix
    has_left, has_right = ix > 0, ix < nx - 1
    at_wall, at_top = iy == 0, iy == ny - 1
    z_low = {"gz": lax.rem(iz + nz - 1, nz)}
    z_high = {"gz": lax.rem(iz + 1, nz)}

    barrier = pltpu.get_barrier_semaphore()

    def greet(target):
        pl.semaphore_signal(barrier, inc=1, device_id=target, device_id_type=MESH)

    is_first, is_second, is_last = iz == 0, iz == 1, iz == nz - 1
    mirror_up = at_wall & (partner > ix)
    mirror_down = at_wall & (partner < ix)
    not_first, not_last = jnp.logical_not(is_first), jnp.logical_not(is_last)
    not_wall, not_top = jnp.logical_not(at_wall), jnp.logical_not(at_top)
    x_low, x_high = {"gx": ix - 1}, {"gx": ix + 1}
    y_low, y_high = {"gy": iy - 1}, {"gy": iy + 1}
    opposite = {"gx": partner}

    def when(condition, action):
        pl.when(condition)(action)

    when(not_last, lambda: greet(z_high))
    when(is_first | is_second, lambda: greet({"gz": nz - 1}))
    when(has_right, lambda: greet(x_high))
    when(not_top, lambda: greet(y_high))
    when(mirror_up, lambda: greet(opposite))
    other_core = lax.rem(iy, 2) == 1
    when(other_core, lambda: greet(y_low))

    as_int = lambda flag: flag.astype(jnp.int32)
    pl.semaphore_wait(
        barrier,
        as_int(not_first)
        + 2 * as_int(is_last)
        + as_int(has_left)
        + as_int(not_wall)
        + as_int(mirror_down)
        + as_int(not_top & jnp.logical_not(other_core)),
    )

    lane = lax.broadcasted_iota(jnp.int32, (rows, lanes), 1)
    sublane = lax.broadcasted_iota(jnp.int32, (rows, lanes), 0)

    def remote(src, dst, index, target):
        return pltpu.make_async_remote_copy(
            src_ref=src,
            dst_ref=dst,
            send_sem=send_sem.at[index],
            recv_sem=recv_sem.at[index],
            device_id=target,
            device_id_type=MESH,
        )

    def up_copy(j):
        return remote(zv.at[:, 2 + planes - j], zv.at[:, 2 - j], Z_UP + j, z_high)

    def down_copy(j):
        return remote(zv.at[:, 3 + j], zv.at[:, 3 + planes + j], Z_DOWN + j, z_low)

    def relay_copy(j):
        return pltpu.make_async_remote_copy(
            src_ref=relay if j == 0 else zv.at[:, j - 1],
            dst_ref=zv.at[:, 3 + planes + j],
            send_sem=send_sem.at[RELAY + j],
            recv_sem=recv_sem.at[Z_DOWN + j],
            device_id={"gz": nz - 1},
            device_id_type=MESH,
        )

    extra = remote(zv.at[:, 3], relay, Z_LAST, z_high)
    ups = [up_copy(j) for j in range(3)]
    downs = [down_copy(j) for j in range(3)]
    relays = [relay_copy(j) for j in range(3)]

    def start(copies):
        def action():
            for copy in copies:
                copy.start()

        return action

    def start_wrap(count):
        for j in count:
            plane = planes - 1 - j
            for part, low, high in ((flow_ref.at[:, plane], 0, 5), (metrics_ref.at[6:9, plane], 5, 8)):
                pltpu.make_async_remote_copy(
                    src_ref=part,
                    dst_ref=zv.at[low:high, 2 - j],
                    send_sem=send_sem.at[Z_UP + j],
                    recv_sem=recv_sem.at[Z_UP + j],
                    device_id=z_high,
                    device_id_type=MESH,
                ).start()

    when(is_last, lambda: start_wrap((0,)))
    when(is_last & jnp.logical_not(other_core), lambda: start_wrap((1, 2)))

    def start_downs():
        for j in range(3):
            for part, low, high in ((flow_ref.at[:, j], 0, 5), (metrics_ref.at[6:9, j], 5, 8)):
                pltpu.make_async_remote_copy(
                    src_ref=part,
                    dst_ref=zv.at[low:high, 3 + planes + j],
                    send_sem=send_sem.at[Z_DOWN + j],
                    recv_sem=recv_sem.at[Z_DOWN + j],
                    device_id=z_low,
                    device_id_type=MESH,
                ).start()

    def y_copies(kind, early):
        flow = flow_ref if early else zv.at[0:5, 3 : 3 + planes]
        row = metrics_ref.at[3:6] if early else ym
        copies = []
        for j in range(3):
            if kind == "down":
                index, target, cell = Y_DOWN + j, {"gy": iy - 1}, j
                flow_dst = lambda lo, hi: yv.at[lo:hi, 7 + j, 4:8, :]
            elif kind == "up":
                index, target, cell = Y_UP + j, {"gy": iy + 1}, rows - 3 + j
                flow_dst = lambda lo, hi: yv.at[lo:hi, j, 0:4, :]
            else:
                index, target, cell = MIRROR + j, {"gx": partner}, j
                flow_dst = lambda lo, hi: mirror.at[lo:hi, j, 0:4, :]
            copies.append(
                pltpu.make_async_remote_copy(
                    src_ref=flow.at[:, :, cell, :],
                    dst_ref=flow_dst(0, 5),
                    send_sem=send_sem.at[index],
                    recv_sem=recv_sem.at[index],
                    device_id=target,
                    device_id_type=MESH,
                )
            )
            copies.append(
                pltpu.make_async_remote_copy(
                    src_ref=row.at[:, :, cell, :],
                    dst_ref=flow_dst(5, 8),
                    send_sem=send_sem.at[N_SEMS + index],
                    recv_sem=recv_sem.at[N_SEMS + index],
                    device_id=target,
                    device_id_type=MESH,
                )
            )
        return copies

    y_down, y_up = y_copies("down", True), y_copies("up", False)
    to_mirror = y_copies("mirror", False)

    when(not_first & not_last, start_downs)
    when(mirror_down, start(y_copies("mirror", True)))
    when(not_wall, start(y_down))
    loads = [
        pltpu.make_async_copy(flow_ref, zv.at[0:5, 3 : 3 + planes], load_sem.at[0]),
        pltpu.make_async_copy(metrics_ref.at[6:9], zv.at[5:8, 3 : 3 + planes], load_sem.at[1]),
        pltpu.make_async_copy(metrics_ref.at[0:3], xm, load_sem.at[2]),
        pltpu.make_async_copy(metrics_ref.at[3:6], ym, load_sem.at[3]),
        pltpu.make_async_copy(wake_ref, wake, load_sem.at[4]),
        pltpu.make_async_copy(inv_ref, inv, load_sem.at[5]),
    ]
    for copy in loads:
        copy.start()

    def tell(index, target):
        pl.semaphore_signal(ready.at[index], inc=1, device_id=target, device_id_type=MESH)

    def hear(index):
        pl.semaphore_wait(ready.at[index], 1)

    when(not_first, lambda: tell(0, z_low))
    when(is_last, lambda: tell(1, {"gz": 1}))
    when(has_left, lambda: tell(2, x_low))
    when(not_wall, lambda: tell(3, y_low))
    when(mirror_down, lambda: tell(4, opposite))

    for copy in loads[0:2]:
        copy.wait()
    for copy in loads[2:]:
        copy.wait()

    def source(c, p):
        return zv[c, 3 + p] if c < 5 else xm[c - 5, p]

    for c in range(8):
        packed = source(c, planes - 1)
        for p in range(planes):
            value = source(c, p)
            low = pltpu.roll(value, 16 * p + 3, 1)
            high = pltpu.roll(value, (16 * p + 13) % lanes, 1)
            packed = jnp.where((lane >= 16 * p + 3) & (lane < 16 * p + 8), low, packed)
            packed = jnp.where((lane >= 16 * p + 8) & (lane < 16 * p + 13), high, packed)
        edge[c] = packed

    x_down = remote(edge, edge_high, X_DOWN, x_low)
    x_up = remote(edge, edge_low, X_UP, x_high)
    when(has_left, x_down.start)

    @pl.when(not_last)
    def _():
        hear(0)
        when(is_first, extra.start)
        start([ups[2], ups[1], ups[0]])()

    @pl.when(mirror_up)
    def _():
        hear(4)
        start(to_mirror)()

    @pl.when(not_top)
    def _():
        hear(3)
        start(y_up)()

    @pl.when(has_right)
    def _():
        hear(2)
        x_up.start()

    def x_plane(p, _):
        when(is_last & other_core & (p == 1), start(ups[1:2]))
        when(is_last & other_core & (p == 2), start(ups[2:]))
        flux = lane_sweep([zv[c, 3 + p] for c in range(5)], [xm[j, p] for j in range(3)], 0)
        for c in range(5):
            x_faces[c, p] = flux[c]
        return _

    lax.fori_loop(0, planes, x_plane, 0)

    @pl.when(is_second)
    def _():
        hear(1)
        for arriving, leaving in zip((extra, ups[2], ups[1]), relays):
            arriving.wait_recv()
            leaving.start()

    when(is_last, start(downs))

    lower_half = sublane < 4
    for c in range(8):
        swapped = swap_blocks(
            [zv[c, 3 + p] if c < 5 else ym[c - 5, p] for p in range(planes)], sublane
        )
        for k in range(4):
            yv[c, 3 + k] = swapped[k]
        for k in range(3):
            yv[c, k, 4:8] = swapped[1 + k][0:4]
            yv[c, 7 + k, 0:4] = swapped[k][4:8]

    prepare_y, face_y = line_steps(yv, terms, faces, 1)
    prepare_z, face_z = line_steps(zv, z_terms, z_faces, 2)
    lax.fori_loop(3, 3 + planes, prepare_z, 0)
    lax.fori_loop(3, 7, prepare_y, 0)

    @pl.when(jnp.logical_not(at_top))
    def _():
        for copy in y_down:
            copy.wait_recv()

    @pl.when(at_top)
    def _():
        for c in range(8):
            for k in range(3):
                yv[c, 7 + k, 4:8] = yv[c, 6, 4:8]

    lax.fori_loop(7, 10, prepare_y, 0)
    lax.fori_loop(3, 5, face_y, 0)

    @pl.when(jnp.logical_not(at_wall))
    def _():
        for copy in y_up:
            copy.wait_recv()

    @pl.when(at_wall)
    def _():
        for copy in to_mirror:
            copy.wait_recv()
        is_wake = jnp.broadcast_to(wake[...], (rows, lanes)) >= 0
        backwards = (lanes - 1) - lane
        for c in range(8):
            for k in range(3):
                facing = jnp.take_along_axis(
                    mirror[c, k], backwards, axis=1, mode="promise_in_bounds"
                )
                here = yv[c, 3 + k]
                if 1 <= c <= 3:
                    here = -here
                yv[c, 2 - k, 0:4] = jnp.where(is_wake, facing, here)[0:4]

    lax.fori_loop(0, 3, prepare_y, 0)
    lax.fori_loop(0, 3, face_y, 0)
    y_parts = []
    for c in range(5):
        y_parts.append(
            swap_blocks([faces[c, k] - faces[c, k + 1] for k in range(4)], sublane)
        )
    for c in range(5):
        for p in range(planes):
            rate_ref[c, p] = y_parts[c][p]

    @pl.when(has_left)
    def _():
        x_up.wait_recv()

    @pl.when(jnp.logical_not(has_left))
    def _():
        for c in range(8):
            for k in range(3):
                moved = pltpu.roll(edge[c], 7 + k, 1)
                edge_low[c] = moved if k == 0 else jnp.where(lane % 16 == 10 + k, moved, edge_low[c])

    @pl.when(has_right)
    def _():
        x_down.wait_recv()

    @pl.when(jnp.logical_not(has_right))
    def _():
        for c in range(8):
            for k in range(3):
                moved = pltpu.roll(edge[c], (3 + k - 12) % lanes, 1)
                edge_high[c] = moved if k == 0 else jnp.where(lane % 16 == 3 + k, moved, edge_high[c])

    place = lane % 16
    ends = []
    for c in range(8):
        value = jnp.where(place < 3, pltpu.roll(edge_low[c], lanes - 10, 1), edge[c])
        value = jnp.where(place >= 13, pltpu.roll(edge_high[c], 10, 1), value)
        ends.append(value)
    ends = lane_sweep(ends[0:5], ends[5:8], 0)
    for c in range(5):
        for p in range(planes):
            low = pltpu.roll(ends[c], (-(16 * p + 3)) % lanes, 1)
            high = pltpu.roll(ends[c], (lanes - 3 - (16 * p + 10)) % lanes, 1)
            upper = jnp.where(lane < 2, low, jnp.where(lane >= lanes - 3, high, x_faces[c, p]))
            lower = pltpu.roll(jnp.where(lane == lanes - 1, low, upper), 1, 1)
            rate_ref[c, p] = rate_ref[c, p] + (lower - upper)

    below_last = 2 * iz < nz
    pick = lambda low, high: jnp.where(below_last, low, high)

    def arrival(slot, index):
        return remote(zv.at[:, 3], zv.at[:, slot], index, z_high)

    def finish(k, _):
        volume = inv[k]
        for c in range(5):
            rate = volume * (rate_ref[c, k] + (z_faces[c, k] - z_faces[c, k + 1]))
            rate_ref[c, k] = rate
            state_ref[c, k] = zv[c, 3 + k] + STEP_SIZE * rate
        return _

    def soon(j, carry):
        slot = pick(7 + j, 2 - j)
        arrival(slot, pick(Z_DOWN + j, Z_UP + j)).wait_recv()
        return prepare_z(slot, carry)

    lax.fori_loop(0, 3, soon, 0)
    lax.fori_loop(0, 2, lambda j, carry: face_z(pick(3 + j, j), carry), 0)
    finish(pick(3, 0), 0)

    def late(j, carry):
        slot = pick(2 - j, 7 + j)

        @pl.when(jnp.logical_not(is_second) | (j == 0))
        def _():
            arrival(slot, pick(Z_UP + j, Z_DOWN + j)).wait_recv()

        prepare_z(slot, 0)
        face_z(pick(2 - j, 2 + j), 0)
        finish(pick(2 - j, 1 + j), 0)
        return carry

    for copy in ups:
        copy.wait_send()

    @pl.when(is_first)
    def _():
        extra.wait_send()

    @pl.when(jnp.logical_not(is_first))
    def _():
        for copy in downs:
            copy.wait_send()

    @pl.when(has_left)
    def _():
        x_down.wait_send()

    @pl.when(has_right)
    def _():
        x_up.wait_send()

    @pl.when(at_wall)
    def _():
        for copy in to_mirror:
            copy.wait_send()

    @pl.when(jnp.logical_not(at_wall))
    def _():
        for copy in y_down:
            copy.wait_send()

    @pl.when(jnp.logical_not(at_top))
    def _():
        for copy in y_up:
            copy.wait_send()

    lax.fori_loop(0, 3, late, 0)

    @pl.when(is_second)
    def _():
        for copy in relays:
            copy.wait_send()


def store(state_ref, rate_ref, state_out, rate_out, sem):
    copies = [
        pltpu.make_async_copy(state_ref, state_out, sem.at[0]),
        pltpu.make_async_copy(rate_ref, rate_out, sem.at[1]),
    ]
    for copy in copies:
        copy.start()
    for copy in copies:
        copy.wait()


def solution(mesh):
    nx, ny, nz = mesh.shape["gx"], mesh.shape["gy"], mesh.shape["gz"]
    assert nz > 2 and nx % 2 == 0

    def local(conserved, metrics, inv_volume, wake_donor):
        planes, rows, lanes = conserved.shape[1:]
        tile = (rows, lanes)
        operands = (conserved, metrics, inv_volume, wake_donor.reshape(1, lanes))
        results = pl.pallas_call(
            functools.partial(kernel, (nx, ny, nz)),
            out_shape=[jax.ShapeDtypeStruct(conserved.shape, F32)] * 2,
            in_specs=[pl.BlockSpec(memory_space=pltpu.HBM)] * 4,
            out_specs=[pl.BlockSpec(memory_space=pltpu.VMEM)] * 2,
            scratch_shapes=[
                pltpu.VMEM((8, planes + 6) + tile, F32),
                pltpu.VMEM((8,) + tile, F32),
                pltpu.VMEM((3, planes) + tile, F32),
                pltpu.VMEM((3, planes) + tile, F32),
                pltpu.VMEM((1, lanes), jnp.int32),
                pltpu.VMEM((planes,) + tile, F32),
                pltpu.VMEM((8, 10) + tile, F32),
                pltpu.VMEM((8, 3) + tile, F32),
                pltpu.VMEM((8,) + tile, F32),
                pltpu.VMEM((8,) + tile, F32),
                pltpu.VMEM((8,) + tile, F32),
                pltpu.VMEM((10, 10) + tile, F32),
                pltpu.VMEM((5, 5) + tile, F32),
                pltpu.VMEM((10, planes + 6) + tile, F32),
                pltpu.VMEM((5, planes + 1) + tile, F32),
                pltpu.VMEM((5, planes) + tile, F32),
                pltpu.SemaphoreType.REGULAR((5,)),
                pltpu.SemaphoreType.DMA((6,)),
                pltpu.SemaphoreType.DMA((2 * N_SEMS,)),
                pltpu.SemaphoreType.DMA((2 * N_SEMS,)),
            ],
            compiler_params=pltpu.CompilerParams(
                collective_id=0, has_side_effects=True, vmem_limit_bytes=8 * 1024 * 1024
            ),
            cost_estimate=pl.CostEstimate(
                flops=60_000_000, bytes_accessed=500_000, transcendentals=0
            ),
        )(*[pltpu.with_memory_space_constraint(x, pltpu.HBM) for x in operands])
        return pl.pallas_call(
            store,
            out_shape=[jax.ShapeDtypeStruct(conserved.shape, F32)] * 2,
            in_specs=[pl.BlockSpec(memory_space=pltpu.VMEM)] * 2,
            out_specs=[pl.BlockSpec(memory_space=pltpu.HBM)] * 2,
            scratch_shapes=[pltpu.SemaphoreType.DMA((2,))],
            compiler_params=pltpu.CompilerParams(vmem_limit_bytes=1024 * 1024),
        )(*results)

    placed = (P(None, "gz", "gy", "gx"), P(None, "gz", "gy", "gx"), P("gz", "gy", "gx"), P("gx"))
    return jax.shard_map(
        local,
        mesh=mesh,
        in_specs=placed,
        out_specs=(P(None, "gz", "gy", "gx"), P(None, "gz", "gy", "gx")),
        check_vma=False,
    )
```

```python
import functools

import jax
import jax.numpy as jnp
from jax import lax
from jax.experimental import pallas as pl
from jax.experimental.pallas import tpu as pltpu
from jax.sharding import PartitionSpec as P

GAMMA = 1.4
WENO_EPS = 1e-06
STEP_SIZE = 0.08
MESH = pl.DeviceIdType.MESH
F32 = jnp.float32

Z_DOWN, Z_UP, Y_DOWN, Y_UP, MIRROR, X_DOWN, X_UP, Z_LAST, RELAY, N_SEMS = 0, 3, 6, 9, 12, 15, 16, 17, 18, 21


def recip(value):
    return 1.0 / value


def dot3(first, second):
    return first[0] * second[0] + first[1] * second[1] + first[2] * second[2]


def cell_terms(flow, row):
    density, momentum, energy = flow[0], flow[1:4], flow[4]
    inverse = recip(density)
    velocity = [part * inverse for part in momentum]
    pressure = (GAMMA - 1.0) * energy - (0.5 * (GAMMA - 1.0)) * dot3(momentum, velocity)
    contra = dot3(row, velocity)
    flux = [density * contra]
    flux += [momentum[j] * contra + row[j] * pressure for j in range(3)]
    flux += [(energy + pressure) * contra]
    squared = (GAMMA * pressure * inverse) * dot3(row, row)
    speed = jnp.abs(contra) + squared * lax.rsqrt(squared)
    return velocity, pressure, flux, speed


def weno_part(d0, d1, d2, d3):
    x0, x1, x2 = d1 - d0, d2 - d1, d3 - d2
    e1, e2 = 0.75 * d1, 0.75 * d2
    eps = 3.0 * WENO_EPS
    b0 = (x0 * x0 + eps) + e1 * (x0 + d1)
    b1 = (x1 * x1 + eps) + e1 * d2
    b2 = (x2 * x2 + eps) + e2 * (d2 - x2)
    t12, t02, t01 = b1 * b2, b0 * b2, b0 * b1
    s12, s02, s01 = t12 * t12, t02 * t02, t01 * t01
    w2 = 1.5 * s01
    total = (s12 + 6.0 * s02) + (w2 + w2)
    top = s12 * (x0 - x1) + w2 * (x1 - x2)
    return top * recip(total)


def face_flux(d_flow, d_flux, flux_low, alpha, state, row, sweep):
    e, a, b = (sweep + 1) % 3, (sweep + 2) % 3, sweep
    density, velocity, pressure = state
    inverse_density = recip(density)
    sound2 = GAMMA * pressure * inverse_density
    inverse_sound = lax.rsqrt(sound2)
    sound = sound2 * inverse_sound
    inverse_size = lax.rsqrt(dot3(row, row))
    normal = [row[j] * inverse_size for j in range(3)]
    cross_size = lax.rsqrt(row[a] * row[a] + row[b] * row[b])
    l_a, l_b = row[b] * cross_size, -(row[a] * cross_size)
    m_e = normal[a] * l_b - normal[b] * l_a
    m_a = -(normal[e] * l_b)
    m_b = normal[e] * l_a
    kinetic = 0.5 * dot3(velocity, velocity)
    half_factor = (0.5 * (GAMMA - 1.0)) * inverse_sound * inverse_sound
    half_normal = [(0.5 * inverse_sound) * normal[j] for j in range(3)]

    def project(vector):
        rho = vector[0]
        w = [vector[1 + j] - velocity[j] * rho for j in range(3)]
        half_a = half_factor * ((vector[4] - kinetic * rho) - dot3(velocity, w))
        half_n = dot3(half_normal, w)
        return [
            half_a - half_n,
            rho - (half_a + half_a),
            l_a * w[a] + l_b * w[b],
            m_e * w[e] + m_a * w[a] + m_b * w[b],
            half_a + half_n,
        ]

    scaled = [[alpha * d_flow(m, c) for c in range(5)] for m in range(5)]
    ups = [[scaled[m][c] + d_flux(m, c) for c in range(5)] for m in range(4)]
    downs = [[scaled[m][c] - d_flux(m, c) for c in range(5)] for m in range(1, 5)]
    up_chars = [project(vector) for vector in ups]
    down_chars = [project(vector) for vector in downs]
    chars = [
        weno_part(*[up_chars[m][r] for m in range(4)])
        + weno_part(*[down_chars[m][r] for m in (3, 2, 1, 0)])
        for r in range(5)
    ]
    both = chars[0] + chars[4]
    carried = sound * (chars[4] - chars[0])
    mass = both + chars[1]
    enthalpy = sound2 * (1.0 / (GAMMA - 1.0)) + kinetic
    tangent_speed = l_a * velocity[a] + l_b * velocity[b]
    binormal_speed = m_e * velocity[e] + m_a * velocity[a] + m_b * velocity[b]
    right = [None] * 5
    right[0] = mass
    right[1 + e] = velocity[e] * mass + normal[e] * carried + m_e * chars[3]
    right[1 + a] = (velocity[a] * mass + normal[a] * carried) + (l_a * chars[2] + m_a * chars[3])
    right[1 + b] = (velocity[b] * mass + normal[b] * carried) + (l_b * chars[2] + m_b * chars[3])
    right[4] = (enthalpy * both + kinetic * chars[1]) + (
        (tangent_speed * chars[2] + binormal_speed * chars[3]) + dot3(normal, velocity) * carried
    )
    return [
        (flux_low[c] + 0.5 * d_flux(2, c))
        + (1.0 / 6.0) * ((0.5 * (ups[1][c] + downs[2][c]) - scaled[2][c]) + right[c])
        for c in range(5)
    ]


def line_steps(cells, terms, faces, sweep):
    def prepare(k, _):
        flow = [cells[c, k] for c in range(5)]
        row = [cells[5 + j, k] for j in range(3)]
        velocity, pressure, flux, speed = cell_terms(flow, row)
        for c in range(5):
            terms[c, k] = flux[c]
        terms[5, k] = speed
        for j in range(3):
            terms[6 + j, k] = velocity[j]
        terms[9, k] = pressure
        return _

    def one_face(k, _):
        alpha = terms[5, k]
        for m in range(1, 6):
            alpha = jnp.maximum(alpha, terms[5, k + m])
        density = 0.5 * (cells[0, k + 2] + cells[0, k + 3])
        velocity = [0.5 * (terms[6 + j, k + 2] + terms[6 + j, k + 3]) for j in range(3)]
        pressure = 0.5 * (terms[9, k + 2] + terms[9, k + 3])
        row = [0.5 * (cells[5 + j, k + 2] + cells[5 + j, k + 3]) for j in range(3)]
        flux = face_flux(
            lambda m, c: cells[c, k + m + 1] - cells[c, k + m],
            lambda m, c: terms[c, k + m + 1] - terms[c, k + m],
            [terms[c, k + 2] for c in range(5)],
            alpha,
            (density, velocity, pressure),
            row,
            sweep,
        )
        for c in range(5):
            faces[c, k] = flux[c]
        return _

    return prepare, one_face


def lane_sweep(flow, row, sweep):
    lanes = flow[0].shape[-1]

    def ahead(value, shift):
        return pltpu.roll(value, (-shift) % lanes, 1)

    velocity, pressure, flux, speed = cell_terms(flow, row)
    pair = jnp.maximum(speed, ahead(speed, 1))
    alpha = jnp.maximum(jnp.maximum(pair, ahead(pair, -2)), ahead(pair, 2))
    mean = lambda value: 0.5 * (value + ahead(value, 1))
    state = (mean(flow[0]), [mean(part) for part in velocity], mean(pressure))
    row_mean = [mean(part) for part in row]
    d_flow = [ahead(part, 1) - part for part in flow]
    d_flux = [ahead(part, 1) - part for part in flux]
    shifted_flow = [[part if m == 2 else ahead(part, m - 2) for part in d_flow] for m in range(5)]
    shifted_flux = [[part if m == 2 else ahead(part, m - 2) for part in d_flux] for m in range(5)]
    return face_flux(
        lambda m, c: shifted_flow[m][c],
        lambda m, c: shifted_flux[m][c],
        flux,
        alpha,
        state,
        row_mean,
        sweep,
    )


def swap_blocks(values, sublane):
    def exchange(first, second, step):
        high = (sublane // step) % 2 == 1
        return (
            jnp.where(high, pltpu.roll(second, step, 0), first),
            jnp.where(high, second, pltpu.roll(first, 8 - step, 0)),
        )

    v0, v1, v2, v3 = values
    v0, v2 = exchange(v0, v2, 2)
    v1, v3 = exchange(v1, v3, 2)
    v0, v1 = exchange(v0, v1, 1)
    v2, v3 = exchange(v2, v3, 1)
    return [v0, v1, v2, v3]


def kernel(
    shape,
    flow_ref,
    metrics_ref,
    inv_ref,
    wake_ref,
    state_ref,
    rate_ref,
    zv,
    relay,
    ym,
    xm,
    wake,
    inv,
    yv,
    mirror,
    edge,
    edge_low,
    edge_high,
    terms,
    faces,
    z_terms,
    z_faces,
    x_faces,
    ready,
    load_sem,
    send_sem,
    recv_sem,
):
    nx, ny, nz = shape
    planes, rows, lanes = flow_ref.shape[1:]
    ix, iy, iz = lax.axis_index("gx"), lax.axis_index("gy"), lax.axis_index("gz")
    partner = nx - 1 - ix
    has_left, has_right = ix > 0, ix < nx - 1
    at_wall, at_top = iy == 0, iy == ny - 1
    z_low = {"gz": lax.rem(iz + nz - 1, nz)}
    z_high = {"gz": lax.rem(iz + 1, nz)}

    barrier = pltpu.get_barrier_semaphore()

    def greet(target):
        pl.semaphore_signal(barrier, inc=1, device_id=target, device_id_type=MESH)

    is_first, is_second, is_last = iz == 0, iz == 1, iz == nz - 1
    mirror_up = at_wall & (partner > ix)
    mirror_down = at_wall & (partner < ix)
    not_first, not_last = jnp.logical_not(is_first), jnp.logical_not(is_last)
    not_wall, not_top = jnp.logical_not(at_wall), jnp.logical_not(at_top)
    x_low, x_high = {"gx": ix - 1}, {"gx": ix + 1}
    y_low, y_high = {"gy": iy - 1}, {"gy": iy + 1}
    opposite = {"gx": partner}

    def when(condition, action):
        pl.when(condition)(action)

    when(not_last, lambda: greet(z_high))
    when(is_first | is_second, lambda: greet({"gz": nz - 1}))
    when(has_right, lambda: greet(x_high))
    when(not_top, lambda: greet(y_high))
    when(mirror_up, lambda: greet(opposite))
    other_core = lax.rem(iy, 2) == 1
    when(other_core, lambda: greet(y_low))

    as_int = lambda flag: flag.astype(jnp.int32)
    pl.semaphore_wait(
        barrier,
        as_int(not_first)
        + 2 * as_int(is_last)
        + as_int(has_left)
        + as_int(not_wall)
        + as_int(mirror_down)
        + as_int(not_top & jnp.logical_not(other_core)),
    )

    lane = lax.broadcasted_iota(jnp.int32, (rows, lanes), 1)
    sublane = lax.broadcasted_iota(jnp.int32, (rows, lanes), 0)

    def remote(src, dst, index, target):
        return pltpu.make_async_remote_copy(
            src_ref=src,
            dst_ref=dst,
            send_sem=send_sem.at[index],
            recv_sem=recv_sem.at[index],
            device_id=target,
            device_id_type=MESH,
        )

    def up_copy(j):
        return remote(zv.at[:, 2 + planes - j], zv.at[:, 2 - j], Z_UP + j, z_high)

    def down_copy(j):
        return remote(zv.at[:, 3 + j], zv.at[:, 3 + planes + j], Z_DOWN + j, z_low)

    def relay_copy(j):
        return pltpu.make_async_remote_copy(
            src_ref=relay if j == 0 else zv.at[:, j - 1],
            dst_ref=zv.at[:, 3 + planes + j],
            send_sem=send_sem.at[RELAY + j],
            recv_sem=recv_sem.at[Z_DOWN + j],
            device_id={"gz": nz - 1},
            device_id_type=MESH,
        )

    extra = remote(zv.at[:, 3], relay, Z_LAST, z_high)
    ups = [up_copy(j) for j in range(3)]
    downs = [down_copy(j) for j in range(3)]
    relays = [relay_copy(j) for j in range(3)]

    def start(copies):
        def action():
            for copy in copies:
                copy.start()

        return action

    def start_wrap(count):
        for j in count:
            plane = planes - 1 - j
            for part, low, high in ((flow_ref.at[:, plane], 0, 5), (metrics_ref.at[6:9, plane], 5, 8)):
                pltpu.make_async_remote_copy(
                    src_ref=part,
                    dst_ref=zv.at[low:high, 2 - j],
                    send_sem=send_sem.at[Z_UP + j],
                    recv_sem=recv_sem.at[Z_UP + j],
                    device_id=z_high,
                    device_id_type=MESH,
                ).start()

    when(is_last, lambda: start_wrap((0,)))
    when(is_last & jnp.logical_not(other_core), lambda: start_wrap((1, 2)))

    def start_downs():
        for j in range(3):
            for part, low, high in ((flow_ref.at[:, j], 0, 5), (metrics_ref.at[6:9, j], 5, 8)):
                pltpu.make_async_remote_copy(
                    src_ref=part,
                    dst_ref=zv.at[low:high, 3 + planes + j],
                    send_sem=send_sem.at[Z_DOWN + j],
                    recv_sem=recv_sem.at[Z_DOWN + j],
                    device_id=z_low,
                    device_id_type=MESH,
                ).start()

    def y_copies(kind, early):
        flow = flow_ref if early else zv.at[0:5, 3 : 3 + planes]
        row = metrics_ref.at[3:6] if early else ym
        copies = []
        for j in range(3):
            if kind == "down":
                index, target, cell = Y_DOWN + j, {"gy": iy - 1}, j
                flow_dst = lambda lo, hi: yv.at[lo:hi, 7 + j, 4:8, :]
            elif kind == "up":
                index, target, cell = Y_UP + j, {"gy": iy + 1}, rows - 3 + j
                flow_dst = lambda lo, hi: yv.at[lo:hi, j, 0:4, :]
            else:
                index, target, cell = MIRROR + j, {"gx": partner}, j
                flow_dst = lambda lo, hi: mirror.at[lo:hi, j, 0:4, :]
            copies.append(
                pltpu.make_async_remote_copy(
                    src_ref=flow.at[:, :, cell, :],
                    dst_ref=flow_dst(0, 5),
                    send_sem=send_sem.at[index],
                    recv_sem=recv_sem.at[index],
                    device_id=target,
                    device_id_type=MESH,
                )
            )
            copies.append(
                pltpu.make_async_remote_copy(
                    src_ref=row.at[:, :, cell, :],
                    dst_ref=flow_dst(5, 8),
                    send_sem=send_sem.at[N_SEMS + index],
                    recv_sem=recv_sem.at[N_SEMS + index],
                    device_id=target,
                    device_id_type=MESH,
                )
            )
        return copies

    y_down, y_up = y_copies("down", True), y_copies("up", False)
    to_mirror = y_copies("mirror", False)

    when(not_first & not_last, start_downs)
    when(mirror_down, start(y_copies("mirror", True)))
    when(not_wall, start(y_down))
    loads = [
        pltpu.make_async_copy(flow_ref, zv.at[0:5, 3 : 3 + planes], load_sem.at[0]),
        pltpu.make_async_copy(metrics_ref.at[6:9], zv.at[5:8, 3 : 3 + planes], load_sem.at[1]),
        pltpu.make_async_copy(metrics_ref.at[0:3], xm, load_sem.at[2]),
        pltpu.make_async_copy(metrics_ref.at[3:6], ym, load_sem.at[3]),
        pltpu.make_async_copy(wake_ref, wake, load_sem.at[4]),
        pltpu.make_async_copy(inv_ref, inv, load_sem.at[5]),
    ]
    for copy in loads:
        copy.start()

    def tell(index, target):
        pl.semaphore_signal(ready.at[index], inc=1, device_id=target, device_id_type=MESH)

    def hear(index):
        pl.semaphore_wait(ready.at[index], 1)

    when(not_first, lambda: tell(0, z_low))
    when(is_last, lambda: tell(1, {"gz": 1}))
    when(has_left, lambda: tell(2, x_low))
    when(not_wall, lambda: tell(3, y_low))
    when(mirror_down, lambda: tell(4, opposite))

    for copy in loads[0:2]:
        copy.wait()
    for copy in loads[2:]:
        copy.wait()

    def source(c, p):
        return zv[c, 3 + p] if c < 5 else xm[c - 5, p]

    for c in range(8):
        packed = source(c, planes - 1)
        for p in range(planes):
            value = source(c, p)
            low = pltpu.roll(value, 16 * p + 3, 1)
            high = pltpu.roll(value, (16 * p + 13) % lanes, 1)
            packed = jnp.where((lane >= 16 * p + 3) & (lane < 16 * p + 8), low, packed)
            packed = jnp.where((lane >= 16 * p + 8) & (lane < 16 * p + 13), high, packed)
        edge[c] = packed

    x_down = remote(edge, edge_high, X_DOWN, x_low)
    x_up = remote(edge, edge_low, X_UP, x_high)
    when(has_left, x_down.start)

    @pl.when(not_last)
    def _():
        hear(0)
        when(is_first, extra.start)
        start([ups[2], ups[1]])()
        when(not_first, ups[0].start)

    @pl.when(mirror_up)
    def _():
        hear(4)
        start(to_mirror)()

    @pl.when(not_top)
    def _():
        hear(3)
        start(y_up)()

    @pl.when(has_right)
    def _():
        hear(2)
        x_up.start()

    def x_plane(p, _):
        when(is_last & other_core & (p == 1), start(ups[1:]))
        flux = lane_sweep([zv[c, 3 + p] for c in range(5)], [xm[j, p] for j in range(3)], 0)
        for c in range(5):
            x_faces[c, p] = flux[c]
        return _

    lax.fori_loop(0, planes, x_plane, 0)
    when(is_first, ups[0].start)

    @pl.when(is_second)
    def _():
        hear(1)
        for arriving, leaving in zip((extra, ups[2], ups[1]), relays):
            arriving.wait_recv()
            leaving.start()

    when(is_last, start(downs))

    lower_half = sublane < 4
    for c in range(8):
        swapped = swap_blocks(
            [zv[c, 3 + p] if c < 5 else ym[c - 5, p] for p in range(planes)], sublane
        )
        for k in range(4):
            yv[c, 3 + k] = swapped[k]
        for k in range(3):
            yv[c, k, 4:8] = swapped[1 + k][0:4]
            yv[c, 7 + k, 0:4] = swapped[k][4:8]

    prepare_y, face_y = line_steps(yv, terms, faces, 1)
    prepare_z, face_z = line_steps(zv, z_terms, z_faces, 2)
    lax.fori_loop(3, 3 + planes, prepare_z, 0)
    lax.fori_loop(3, 7, prepare_y, 0)

    @pl.when(jnp.logical_not(at_top))
    def _():
        for copy in y_down:
            copy.wait_recv()

    @pl.when(at_top)
    def _():
        for c in range(8):
            for k in range(3):
                yv[c, 7 + k, 4:8] = yv[c, 6, 4:8]

    lax.fori_loop(7, 10, prepare_y, 0)
    lax.fori_loop(3, 5, face_y, 0)

    @pl.when(jnp.logical_not(at_wall))
    def _():
        for copy in y_up:
            copy.wait_recv()

    @pl.when(at_wall)
    def _():
        for copy in to_mirror:
            copy.wait_recv()
        is_wake = jnp.broadcast_to(wake[...], (rows, lanes)) >= 0
        backwards = (lanes - 1) - lane
        for c in range(8):
            for k in range(3):
                facing = jnp.take_along_axis(
                    mirror[c, k], backwards, axis=1, mode="promise_in_bounds"
                )
                here = yv[c, 3 + k]
                if 1 <= c <= 3:
                    here = -here
                yv[c, 2 - k, 0:4] = jnp.where(is_wake, facing, here)[0:4]

    lax.fori_loop(0, 3, prepare_y, 0)
    lax.fori_loop(0, 3, face_y, 0)
    y_parts = []
    for c in range(5):
        y_parts.append(
            swap_blocks([faces[c, k] - faces[c, k + 1] for k in range(4)], sublane)
        )
    for c in range(5):
        for p in range(planes):
            rate_ref[c, p] = y_parts[c][p]

    @pl.when(has_left)
    def _():
        x_up.wait_recv()

    @pl.when(jnp.logical_not(has_left))
    def _():
        for c in range(8):
            for k in range(3):
                moved = pltpu.roll(edge[c], 7 + k, 1)
                edge_low[c] = moved if k == 0 else jnp.where(lane % 16 == 10 + k, moved, edge_low[c])

    @pl.when(has_right)
    def _():
        x_down.wait_recv()

    @pl.when(jnp.logical_not(has_right))
    def _():
        for c in range(8):
            for k in range(3):
                moved = pltpu.roll(edge[c], (3 + k - 12) % lanes, 1)
                edge_high[c] = moved if k == 0 else jnp.where(lane % 16 == 3 + k, moved, edge_high[c])

    place = lane % 16
    ends = []
    for c in range(8):
        value = jnp.where(place < 3, pltpu.roll(edge_low[c], lanes - 10, 1), edge[c])
        value = jnp.where(place >= 13, pltpu.roll(edge_high[c], 10, 1), value)
        ends.append(value)
    ends = lane_sweep(ends[0:5], ends[5:8], 0)
    for c in range(5):
        for p in range(planes):
            low = pltpu.roll(ends[c], (-(16 * p + 3)) % lanes, 1)
            high = pltpu.roll(ends[c], (lanes - 3 - (16 * p + 10)) % lanes, 1)
            upper = jnp.where(lane < 2, low, jnp.where(lane >= lanes - 3, high, x_faces[c, p]))
            lower = pltpu.roll(jnp.where(lane == lanes - 1, low, upper), 1, 1)
            rate_ref[c, p] = rate_ref[c, p] + (lower - upper)

    below_last = 2 * iz < nz
    pick = lambda low, high: jnp.where(below_last, low, high)

    def arrival(slot, index):
        return remote(zv.at[:, 3], zv.at[:, slot], index, z_high)

    def finish(k, _):
        volume = inv[k]
        for c in range(5):
            rate = volume * (rate_ref[c, k] + (z_faces[c, k] - z_faces[c, k + 1]))
            rate_ref[c, k] = rate
            state_ref[c, k] = zv[c, 3 + k] + STEP_SIZE * rate
        return _

    def soon(j, carry):
        slot = pick(7 + j, 2 - j)
        arrival(slot, pick(Z_DOWN + j, Z_UP + j)).wait_recv()
        return prepare_z(slot, carry)

    lax.fori_loop(0, 3, soon, 0)
    lax.fori_loop(0, 2, lambda j, carry: face_z(pick(3 + j, j), carry), 0)
    finish(pick(3, 0), 0)

    def late(j, carry):
        slot = pick(2 - j, 7 + j)

        @pl.when(jnp.logical_not(is_second) | (j == 0))
        def _():
            arrival(slot, pick(Z_UP + j, Z_DOWN + j)).wait_recv()

        prepare_z(slot, 0)
        face_z(pick(2 - j, 2 + j), 0)
        finish(pick(2 - j, 1 + j), 0)
        return carry

    for copy in ups:
        copy.wait_send()

    @pl.when(is_first)
    def _():
        extra.wait_send()

    @pl.when(jnp.logical_not(is_first))
    def _():
        for copy in downs:
            copy.wait_send()

    @pl.when(has_left)
    def _():
        x_down.wait_send()

    @pl.when(has_right)
    def _():
        x_up.wait_send()

    @pl.when(at_wall)
    def _():
        for copy in to_mirror:
            copy.wait_send()

    @pl.when(jnp.logical_not(at_wall))
    def _():
        for copy in y_down:
            copy.wait_send()

    @pl.when(jnp.logical_not(at_top))
    def _():
        for copy in y_up:
            copy.wait_send()

    lax.fori_loop(0, 3, late, 0)

    @pl.when(is_second)
    def _():
        for copy in relays:
            copy.wait_send()


def store(state_ref, rate_ref, state_out, rate_out, sem):
    copies = [
        pltpu.make_async_copy(state_ref, state_out, sem.at[0]),
        pltpu.make_async_copy(rate_ref, rate_out, sem.at[1]),
    ]
    for copy in copies:
        copy.start()
    for copy in copies:
        copy.wait()


def solution(mesh):
    nx, ny, nz = mesh.shape["gx"], mesh.shape["gy"], mesh.shape["gz"]

    def local(conserved, metrics, inv_volume, wake_donor):
        planes, rows, lanes = conserved.shape[1:]
        tile = (rows, lanes)
        operands = (conserved, metrics, inv_volume, wake_donor.reshape(1, lanes))
        results = pl.pallas_call(
            functools.partial(kernel, (nx, ny, nz)),
            out_shape=[jax.ShapeDtypeStruct(conserved.shape, F32)] * 2,
            in_specs=[pl.BlockSpec(memory_space=pltpu.HBM)] * 4,
            out_specs=[pl.BlockSpec(memory_space=pltpu.VMEM)] * 2,
            scratch_shapes=[
                pltpu.VMEM((8, planes + 6) + tile, F32),
                pltpu.VMEM((8,) + tile, F32),
                pltpu.VMEM((3, planes) + tile, F32),
                pltpu.VMEM((3, planes) + tile, F32),
                pltpu.VMEM((1, lanes), jnp.int32),
                pltpu.VMEM((planes,) + tile, F32),
                pltpu.VMEM((8, 10) + tile, F32),
                pltpu.VMEM((8, 3) + tile, F32),
                pltpu.VMEM((8,) + tile, F32),
                pltpu.VMEM((8,) + tile, F32),
                pltpu.VMEM((8,) + tile, F32),
                pltpu.VMEM((10, 10) + tile, F32),
                pltpu.VMEM((5, 5) + tile, F32),
                pltpu.VMEM((10, planes + 6) + tile, F32),
                pltpu.VMEM((5, planes + 1) + tile, F32),
                pltpu.VMEM((5, planes) + tile, F32),
                pltpu.SemaphoreType.REGULAR((5,)),
                pltpu.SemaphoreType.DMA((6,)),
                pltpu.SemaphoreType.DMA((2 * N_SEMS,)),
                pltpu.SemaphoreType.DMA((2 * N_SEMS,)),
            ],
            compiler_params=pltpu.CompilerParams(
                collective_id=0, has_side_effects=True, vmem_limit_bytes=8 * 1024 * 1024
            ),
            cost_estimate=pl.CostEstimate(
                flops=60_000_000, bytes_accessed=500_000, transcendentals=0
            ),
        )(*[pltpu.with_memory_space_constraint(x, pltpu.HBM) for x in operands])
        return pl.pallas_call(
            store,
            out_shape=[jax.ShapeDtypeStruct(conserved.shape, F32)] * 2,
            in_specs=[pl.BlockSpec(memory_space=pltpu.VMEM)] * 2,
            out_specs=[pl.BlockSpec(memory_space=pltpu.HBM)] * 2,
            scratch_shapes=[pltpu.SemaphoreType.DMA((2,))],
            compiler_params=pltpu.CompilerParams(vmem_limit_bytes=1024 * 1024),
        )(*results)

    placed = (P(None, "gz", "gy", "gx"), P(None, "gz", "gy", "gx"), P("gz", "gy", "gx"), P("gx"))
    return jax.shard_map(
        local,
        mesh=mesh,
        in_specs=placed,
        out_specs=(P(None, "gz", "gy", "gx"), P(None, "gz", "gy", "gx")),
        check_vma=False,
    )
```
